8 devices in a mesh: dp: 1 (over z), tp: 2 (over y), cp: 4 (over x, core).
Axes of the slice: x: 2, y: 2, z: 1, core: 2. Of those that a mesh axis runs over, the one named last changes fastest.
Arguments:
- x_chunk: bfloat16 [32, 128, 4096], P('dp', 'cp')
- w_query: bfloat16 [4096, 4096], P(None, 'tp')
- w_key: bfloat16 [4096, 4096], P(None, 'tp')
- w_value: bfloat16 [4096, 4096], P(None, 'tp')
- w_out: bfloat16 [4096, 4096], P('tp')
- q_gain: bfloat16 [4096], P('tp')
- k_gain: bfloat16 [4096], P('tp')
- post_gain: bfloat16 [4096], replicated
- cache_k: bfloat16 [32, 1024, 32, 128], P('dp', 'cp', 'tp')
- cache_v: bfloat16 [32, 1024, 32, 128], P('dp', 'cp', 'tp')
- prefix_len: int32 [32], P('dp')
Outputs:
- output 1: bfloat16 [32, 128, 4096], P('dp', 'cp')
- output 2: bfloat16 [32, 128, 32, 128], P('dp', 'cp', 'tp')
- output 3: bfloat16 [32, 128, 32, 128], P('dp', 'cp', 'tp')
All inputs are finite; a program needn't handle non-finite values.
Results may differ from the reference program's by a relative error of at most 0.0065922.
Values are sent between devices in bfloat16 or wider.
A program may use at most 1 GiB of HBM per device.

```python
import jax
import jax.numpy as jnp
from jax import lax

BATCH_ROWS = 32
CHUNK_LEN = 128
CACHE_LEN = 1024
MODEL_DIM = 4096
Q_HEADS = 32
KV_HEADS = 32
HEAD_DIM = 128
QUERY_BLOCK = min(CHUNK_LEN, 16)
ROPE_BASE = 500000.0
NORM_EPS = 1e-6


def head_scales(rng_key, n_heads, trend_slope):
    trend_pos = jnp.arange(n_heads, dtype=jnp.float32) * (2.0 / max(n_heads - 1, 1)) - 1.0
    noise_val = jax.random.normal(rng_key, (n_heads,), jnp.float32)
    return jnp.exp(trend_slope * trend_pos + 0.2 * noise_val)


def draw_prefix(rng_key):
    key_order, key_len = jax.random.split(rng_key)
    row_order = jax.random.permutation(key_order, BATCH_ROWS)
    lengths = jax.random.randint(key_len, (BATCH_ROWS,), CACHE_LEN // 2, CACHE_LEN + 1)
    lengths = jnp.where(row_order == 0, CACHE_LEN, jnp.where(row_order == 1, CACHE_LEN // 2, lengths))
    return lengths.astype(jnp.int32)


def setup_inputs(seed: int = 0, part: int = 0) -> dict:
    shared_keys = jax.random.split(jax.random.key(seed), 9)
    own_keys = jax.random.split(jax.random.fold_in(jax.random.key(seed + 1), part), 4)
    q_width = Q_HEADS * HEAD_DIM
    kv_width = KV_HEADS * HEAD_DIM
    q_cols = jnp.repeat(head_scales(shared_keys[0], Q_HEADS, 0.5), HEAD_DIM)
    k_cols = jnp.repeat(head_scales(shared_keys[1], KV_HEADS, 0.5), HEAD_DIM)
    w_query = jax.random.normal(shared_keys[2], (MODEL_DIM, q_width), jnp.float32) * (MODEL_DIM ** -0.5) * q_cols[None, :]
    w_key = jax.random.normal(shared_keys[3], (MODEL_DIM, kv_width), jnp.float32) * (MODEL_DIM ** -0.5) * k_cols[None, :]
    w_value = jax.random.normal(shared_keys[4], (MODEL_DIM, kv_width), jnp.float32) * (MODEL_DIM ** -0.5)
    w_out = jax.random.normal(shared_keys[5], (q_width, MODEL_DIM), jnp.float32) * (q_width ** -0.5)
    q_gain = 1.0 + 0.25 * jax.random.normal(shared_keys[6], (q_width,), jnp.float32)
    k_gain = 1.0 + 0.25 * jax.random.normal(shared_keys[7], (kv_width,), jnp.float32)
    post_gain = 1.0 + 0.3 * jax.random.normal(shared_keys[8], (MODEL_DIM,), jnp.float32)
    prefix_len = draw_prefix(own_keys[0])
    x_chunk = jax.random.normal(own_keys[1], (BATCH_ROWS, CHUNK_LEN, MODEL_DIM), jnp.float32)
    stale_mask = jnp.arange(CACHE_LEN)[None, :] >= prefix_len[:, None]
    slot_scale = jnp.where(stale_mask, 3.0, 1.0)[:, :, None, None]
    cache_k = 0.8 * jax.random.normal(own_keys[2], (BATCH_ROWS, CACHE_LEN, KV_HEADS, HEAD_DIM), jnp.float32) * slot_scale
    cache_v = jax.random.normal(own_keys[3], (BATCH_ROWS, CACHE_LEN, KV_HEADS, HEAD_DIM), jnp.float32) * slot_scale
    return {
        'x_chunk': x_chunk.astype(jnp.bfloat16),
        'w_query': w_query.astype(jnp.bfloat16),
        'w_key': w_key.astype(jnp.bfloat16),
        'w_value': w_value.astype(jnp.bfloat16),
        'w_out': w_out.astype(jnp.bfloat16),
        'q_gain': q_gain.astype(jnp.bfloat16),
        'k_gain': k_gain.astype(jnp.bfloat16),
        'post_gain': post_gain.astype(jnp.bfloat16),
        'cache_k': cache_k.astype(jnp.bfloat16),
        'cache_v': cache_v.astype(jnp.bfloat16),
        'prefix_len': prefix_len,
    }


def rms_norm(raw_vals, gain_vec):
    mean_sq = jnp.mean(raw_vals * raw_vals, axis=-1, keepdims=True)
    return raw_vals * lax.rsqrt(mean_sq + NORM_EPS) * gain_vec.astype(jnp.float32)


def rope_apply(head_vals, positions):
    half_dim = HEAD_DIM // 2
    inv_freq = ROPE_BASE ** (-(jnp.arange(half_dim, dtype=jnp.float32) * 2.0 / HEAD_DIM))
    angles = positions.astype(jnp.float32)[..., None] * inv_freq
    cos_tab = jnp.cos(angles)[..., None, :]
    sin_tab = jnp.sin(angles)[..., None, :]
    first_half = head_vals[..., :half_dim]
    second_half = head_vals[..., half_dim:]
    return jnp.concatenate([first_half * cos_tab - second_half * sin_tab, second_half * cos_tab + first_half * sin_tab], axis=-1)


def reference(x_chunk, w_query, w_key, w_value, w_out, q_gain, k_gain, post_gain, cache_k, cache_v, prefix_len):
    groups = Q_HEADS // KV_HEADS
    tokens = x_chunk.reshape(BATCH_ROWS * CHUNK_LEN, MODEL_DIM)
    q_raw = jnp.dot(tokens, w_query, preferred_element_type=jnp.float32)
    k_raw = jnp.dot(tokens, w_key, preferred_element_type=jnp.float32)
    v_raw = jnp.dot(tokens, w_value, preferred_element_type=jnp.float32)
    positions = prefix_len[:, None] + jnp.arange(CHUNK_LEN, dtype=jnp.int32)[None, :]
    q_rot = rope_apply(rms_norm(q_raw, q_gain).reshape(BATCH_ROWS, CHUNK_LEN, Q_HEADS, HEAD_DIM), positions)
    k_rot = rope_apply(rms_norm(k_raw, k_gain).reshape(BATCH_ROWS, CHUNK_LEN, KV_HEADS, HEAD_DIM), positions)
    q_new = q_rot.astype(jnp.bfloat16).reshape(BATCH_ROWS, CHUNK_LEN, KV_HEADS, groups, HEAD_DIM)
    chunk_k = k_rot.astype(jnp.bfloat16)
    chunk_v = v_raw.astype(jnp.bfloat16).reshape(BATCH_ROWS, CHUNK_LEN, KV_HEADS, HEAD_DIM)
    key_index = jnp.arange(CACHE_LEN + CHUNK_LEN)
    score_scale = HEAD_DIM ** -0.5

    def row_attention(row_in):
        q_row, k_row, v_row, ck_row, cv_row, valid_len = row_in
        all_keys = jnp.concatenate([ck_row, k_row], axis=0).astype(jnp.float32)
        all_values = jnp.concatenate([cv_row, v_row], axis=0).astype(jnp.float32)
        q_blocks = q_row.reshape(CHUNK_LEN // QUERY_BLOCK, QUERY_BLOCK, KV_HEADS, groups, HEAD_DIM).astype(jnp.float32)

        def block_attention(block_in):
            q_blk, block_id = block_in
            q_index = block_id * QUERY_BLOCK + jnp.arange(QUERY_BLOCK)
            allowed = jnp.where(key_index[None, :] < CACHE_LEN, key_index[None, :] < valid_len, key_index[None, :] - CACHE_LEN <= q_index[:, None])
            scores = jnp.einsum('qkgd,tkd->qkgt', q_blk, all_keys) * score_scale
            scores = jnp.where(allowed[:, None, None, :], scores, -jnp.inf)
            probs_f = jax.nn.softmax(scores, axis=-1)
            return jnp.einsum('qkgt,tkd->qkgd', probs_f, all_values)

        blocks = lax.map(block_attention, (q_blocks, jnp.arange(CHUNK_LEN // QUERY_BLOCK)))
        return blocks.reshape(CHUNK_LEN, Q_HEADS * HEAD_DIM)

    attn_out = lax.map(row_attention, (q_new, chunk_k, chunk_v, cache_k, cache_v, prefix_len))
    attn_out = attn_out.astype(jnp.bfloat16).reshape(BATCH_ROWS * CHUNK_LEN, Q_HEADS * HEAD_DIM)
    mixed_sum = jnp.dot(attn_out, w_out, preferred_element_type=jnp.float32)
    result = x_chunk.astype(jnp.float32) + rms_norm(mixed_sum, post_gain).reshape(BATCH_ROWS, CHUNK_LEN, MODEL_DIM)
    return result.astype(jnp.bfloat16), chunk_k, chunk_v
```

```python
import functools

import jax
import jax.numpy as jnp
from jax import lax
from jax.experimental import pallas as pl
from jax.experimental.pallas import tpu as pltpu
from jax.sharding import PartitionSpec as P

NORM_EPS = 1e-6
ROPE_BASE = 500000.0
NEG = -1e30
FLOOR = -5e29
LOG2E = 1.4426950408889634
HD = 128
LAG = 1
GROUPS = (4, 8, 8, 8, 4)
P_GROUPS = (3, 1, 1)
VMEM_LIMIT = 60 * 1024 * 1024


def cost(micros, moved):
    return pl.CostEstimate(flops=int(micros * 9e8), bytes_accessed=moved, transcendentals=0)


def params():
    return pltpu.CompilerParams(dimension_semantics=("arbitrary",), vmem_limit_bytes=VMEM_LIMIT)


def rope_body(total_width, n_heads, raw, own, peer, gain, cos, sin, out):
    inv = lax.rsqrt((own[...] + peer[...]) / total_width + NORM_EPS)
    inv = jnp.broadcast_to(inv, (HD, HD)).T
    cos_t = cos[...]
    sin_t = sin[...]
    for h in range(n_heads):
        cols = slice(h * HD, (h + 1) * HD)
        u = raw[:, cols] * inv * gain[:, cols]
        out[:, cols] = (u * cos_t + pltpu.roll(u, HD // 2, 1) * sin_t).astype(jnp.bfloat16)


def rope(raw, own, peer, gain, cos, sin, row0, total_width, tokens, raw_row0):
    width = raw.shape[1]
    block = 128
    base = row0 // block
    off = (row0 - raw_row0) // block
    return pl.pallas_call(
        functools.partial(rope_body, total_width, width // HD),
        grid=(tokens // block,),
        in_specs=[pl.BlockSpec((block, width), lambda i: (i + off, 0)),
                  pl.BlockSpec((1, block), lambda i: (0, i + off)),
                  pl.BlockSpec((1, block), lambda i: (0, i + off)),
                  pl.BlockSpec((1, width), lambda i: (0, 0)),
                  pl.BlockSpec((block, HD), lambda i: (i + base, 0)),
                  pl.BlockSpec((block, HD), lambda i: (i + base, 0))],
        out_specs=pl.BlockSpec((block, width), lambda i: (i, 0)),
        out_shape=jax.ShapeDtypeStruct((tokens, width), jnp.bfloat16),
        compiler_params=params(),
        cost_estimate=cost(tokens * 0.005, tokens * width * 6),
        name="rope",
    )(raw, own, peer, gain, cos, sin)


def attn_body(n_heads, row0, chunk, slots, pitch, sc_ref, qa, qb, qc, qd, ck, cv, kc, vc, keep, give, stat, ks, vs):
    b = pl.program_id(0)
    cp = sc_ref[0]
    valid_len = sc_ref[1 + row0 + b]
    tokens = 4 * chunk
    keys = slots + chunk
    for t in range(slots):
        ks[t * pitch:t * pitch + n_heads, :] = ck[0, t].astype(jnp.float32)
        vs[t * pitch:t * pitch + n_heads, :] = cv[0, t].astype(jnp.float32)
    row = lax.broadcasted_iota(jnp.int32, (keys, tokens), 0)
    col = lax.broadcasted_iota(jnp.int32, (keys, tokens), 1)
    part = col // chunk
    rel = jnp.where(part == 1, 2, jnp.where(part == 2, 1, part))
    query = jnp.bitwise_xor(rel, cp) * chunk + col % chunk
    chunk_key = cp * chunk + row - slots
    ok = jnp.where(row < slots, row + cp * slots - valid_len, chunk_key - query - 1) < 0
    scale = HD ** -0.5 * LOG2E
    contract_last = (((1,), (1,)), ((), ()))
    contract_first = (((0,), (0,)), ((), ()))

    def cols(h):
        return slice(h * HD, (h + 1) * HD)

    def scores(h):
        q = jnp.concatenate([qa[0, :, cols(h)], qb[0, :, cols(h)], qc[0, :, cols(h)], qd[0, :, cols(h)]], axis=0)
        k = jnp.concatenate([ks[pl.ds(h, slots, stride=pitch), :].astype(jnp.bfloat16), kc[0, :, cols(h)]], axis=0)
        return lax.dot_general(k, q, contract_last, preferred_element_type=jnp.float32)

    def soft(h, s):
        s = jnp.where(ok, s * scale, NEG)
        top = jnp.maximum(jnp.max(s, axis=0, keepdims=True), FLOOR)
        p = jnp.exp2(s - top)
        stat[0, h:h + 1, :] = top
        stat[0, n_heads + h:n_heads + h + 1, :] = jnp.sum(p, axis=0, keepdims=True)
        return p.astype(jnp.bfloat16)

    def values(h, p):
        v = jnp.concatenate([vs[pl.ds(h, slots, stride=pitch), :].astype(jnp.bfloat16), vc[0, :, cols(h)]], axis=0)
        num = lax.dot_general(p, v, contract_first, preferred_element_type=jnp.float32)
        keep[0, :, cols(h)] = num[:2 * chunk]
        give[0, :, cols(h)] = num[2 * chunk:]

    s_live, p_live = {}, {}
    for step in range(n_heads + 2 * LAG):
        if step < n_heads:
            s_live[step] = scores(step)
        h = step - LAG
        if 0 <= h < n_heads:
            p_live[h] = soft(h, s_live.pop(h))
        h = step - 2 * LAG
        if 0 <= h < n_heads:
            values(h, p_live.pop(h))


def attention(scalars, q_parts, cache_k, cache_v, k_new, v_new, row0):
    rows, chunk, width = q_parts[0].shape
    _, slots, n_heads, _ = cache_k.shape
    pitch = n_heads + 8
    q_spec = pl.BlockSpec((1, chunk, width), lambda b, s: (b, 0, 0))
    new_spec = pl.BlockSpec((1, chunk, width), lambda b, s: (b + row0, 0, 0))
    cache_spec = pl.BlockSpec((1, slots, n_heads, HD), lambda b, s: (b + row0, 0, 0, 0))
    out_spec = pl.BlockSpec((1, 2 * chunk, width), lambda b, s: (b, 0, 0))
    stat_spec = pl.BlockSpec((1, 2 * n_heads, 4 * chunk), lambda b, s: (b, 0, 0))
    out = jax.ShapeDtypeStruct((rows, 2 * chunk, width), jnp.float32)
    return pl.pallas_call(
        functools.partial(attn_body, n_heads, row0, chunk, slots, pitch),
        grid_spec=pltpu.PrefetchScalarGridSpec(
            num_scalar_prefetch=1, grid=(rows,),
            in_specs=[q_spec] * 4 + [cache_spec] * 2 + [new_spec] * 2,
            out_specs=[out_spec] * 2 + [stat_spec],
            scratch_shapes=[pltpu.VMEM((slots * pitch, HD), jnp.float32)] * 2),
        out_shape=[out, out, jax.ShapeDtypeStruct((rows, 2 * n_heads, 4 * chunk), jnp.float32)],
        compiler_params=params(),
        cost_estimate=cost(rows * 3.9, rows * slots * width * 6),
        name="attention",
    )(scalars, *q_parts, cache_k, cache_v, k_new, v_new)


def pair_weights(n_heads, mine, theirs):
    theirs = pltpu.roll(theirs, mine.shape[1] // 2, 1)
    return [(s[:n_heads], s[n_heads:]) for s in (mine, theirs)]


def merge_body(n_heads, chunk, span, keep, got, stat, gstat, out, ostat):
    packed = jnp.zeros((2 * n_heads, 4 * chunk), jnp.float32)
    lane = lax.broadcasted_iota(jnp.int32, (2 * n_heads, 4 * chunk), 1) // chunk
    for i in range(span):
        (t0, d0), (t1, d1) = pair_weights(n_heads, stat[i], gstat[i])
        top = jnp.maximum(t0, t1)
        w0 = jnp.exp2(t0 - top)
        w1 = jnp.exp2(t1 - top)
        new = jnp.concatenate([top, w0 * d0 + w1 * d1], axis=0)
        packed = jnp.where(lane == i, pltpu.roll(new, ((i - 1) * chunk) % (4 * chunk), 1), packed)
        w = jnp.concatenate([w0, w1], axis=0).T[chunk:2 * chunk]
        for h in range(n_heads):
            cols = slice(h * HD, (h + 1) * HD)
            out[i, :, cols] = keep[i, :, cols] * w[:, h:h + 1] + got[i, :, cols] * w[:, n_heads + h:n_heads + h + 1]
    ostat[0] = packed


def merge(keep, got, stat, gstat, n_heads):
    rows, chunk2, width = keep.shape
    chunk = chunk2 // 2
    span = 4
    half = pl.BlockSpec((span, chunk, width), lambda i: (i, 1, 0))
    stats = pl.BlockSpec((span, 2 * n_heads, 4 * chunk), lambda i: (i, 0, 0))
    return pl.pallas_call(
        functools.partial(merge_body, n_heads, chunk, span),
        grid=(rows // span,),
        in_specs=[half, half, stats, stats],
        out_specs=[pl.BlockSpec((span, chunk, width), lambda i: (i, 0, 0)),
                   pl.BlockSpec((1, 2 * n_heads, 4 * chunk), lambda i: (i, 0, 0))],
        out_shape=[jax.ShapeDtypeStruct((rows, chunk, width), jnp.float32),
                   jax.ShapeDtypeStruct((rows // span, 2 * n_heads, 4 * chunk), jnp.float32)],
        compiler_params=params(),
        cost_estimate=cost(rows * 0.3, rows * chunk * width * 12),
        name="merge",
    )(keep, got, stat, gstat)


def finish_body(n_heads, chunk, span, keep, got, far, stat, gstat, fstat, out):
    for i in range(span):
        pairs = pair_weights(n_heads, stat[i], gstat[i])
        third = pltpu.roll(fstat[0], (-i * chunk) % (4 * chunk), 1)
        pairs.append((third[:n_heads], third[n_heads:]))
        top = jnp.maximum(jnp.maximum(pairs[0][0], pairs[1][0]), pairs[2][0])
        ws = [jnp.exp2(t - top) for t, _ in pairs]
        den = ws[0] * pairs[0][1] + ws[1] * pairs[1][1] + ws[2] * pairs[2][1]
        inv = 1.0 / den
        w = jnp.concatenate([x * inv for x in ws], axis=0).T[:chunk]
        for h in range(n_heads):
            cols = slice(h * HD, (h + 1) * HD)
            val = keep[i, :, cols] * w[:, h:h + 1]
            val = val + got[i, :, cols] * w[:, n_heads + h:n_heads + h + 1]
            val = val + far[i, :, cols] * w[:, 2 * n_heads + h:2 * n_heads + h + 1]
            out[i, :, cols] = val.astype(jnp.bfloat16)


def finish(keep, got, far, stat, gstat, fstat, n_heads):
    rows, chunk2, width = keep.shape
    chunk = chunk2 // 2
    span = 4
    half = pl.BlockSpec((span, chunk, width), lambda i: (i, 0, 0))
    stats = pl.BlockSpec((span, 2 * n_heads, 4 * chunk), lambda i: (i, 0, 0))
    return pl.pallas_call(
        functools.partial(finish_body, n_heads, chunk, span),
        grid=(rows // span,),
        in_specs=[half, half, half, stats, stats, pl.BlockSpec((1, 2 * n_heads, 4 * chunk), lambda i: (i, 0, 0))],
        out_specs=half,
        out_shape=jax.ShapeDtypeStruct((rows, chunk, width), jnp.bfloat16),
        compiler_params=params(),
        cost_estimate=cost(rows * 0.4, rows * chunk * width * 14),
        name="finish",
    )(keep, got, far, stat, gstat, fstat)


def project_body(half, steps, block, sizes, row0, sc_ref, *refs):
    n = len(sizes)
    o_in, ro_in = refs[:n], refs[n:2 * n]
    w_own, w_near, w_far, x_hbm, gain = refs[2 * n:2 * n + 5]
    out_hbm, o, ro, x, acc, ssq, sem, out_sem = refs[-8:]
    j = pl.program_id(0)
    core = sc_ref[0] % 2
    tp = sc_ref[1]
    first = pl.multiple_of(core * half, half)
    second = pl.multiple_of((1 - core) * half, half)
    f32 = jnp.float32
    tokens = sum(sizes)
    residual = pltpu.make_async_copy(x_hbm.at[pl.ds(row0, tokens)], x, sem)

    @pl.when(j == 0)
    def _():
        residual.start()
        at = 0
        for k, size in enumerate(sizes):
            o[at:at + size, :] = o_in[k][...]
            ro[at:at + size, :] = ro_in[k][...]
            at += size

    def own():
        return (jnp.dot(o[:, pl.ds(first, half)], w_own[pl.ds(first, half), :], preferred_element_type=f32)
                + jnp.dot(o[:, pl.ds(second, half)], w_own[pl.ds(second, half), :], preferred_element_type=f32))

    def peer():
        return (jnp.dot(ro[:, pl.ds(first, half)], w_near[...], preferred_element_type=f32)
                + jnp.dot(ro[:, pl.ds(second, half)], w_far[...], preferred_element_type=f32))

    def put(a):
        acc[j] = a
        sq = jnp.sum(a * a, axis=-1, keepdims=True)
        ssq[...] = jnp.where(j == 0, sq, ssq[...] + sq)

    @pl.when(tp == 0)
    def _():
        put(own() + peer())

    @pl.when(tp != 0)
    def _():
        put(peer() + own())

    @pl.when(j == steps - 1)
    def _():
        residual.wait()
        inv = lax.rsqrt(ssq[...] / (steps * block) + NORM_EPS)
        for k in range(steps):
            cols = slice(k * block, (k + 1) * block)
            y = x[:, cols].astype(f32) + acc[k] * inv * gain[:, cols].astype(f32)
            x[:, cols] = y.astype(jnp.bfloat16)
        result = pltpu.make_async_copy(x, out_hbm.at[pl.ds(row0, tokens)], out_sem)
        result.start()
        result.wait()


def project(scalars, o_list, ro_list, w_own, w_near, w_far, x, gain, row0, so_far):
    sizes = tuple(o.shape[0] for o in o_list)
    tokens, width = sum(sizes), o_list[0].shape[1]
    half = width // 2
    model = w_own.shape[1]
    block = 512
    steps = model // block
    once = pl.Buffered(1)
    extra = [] if so_far is None else [so_far]
    o_specs = [pl.BlockSpec((size, width), lambda j, s: (0, 0), pipeline_mode=once) for size in sizes]
    return pl.pallas_call(
        functools.partial(project_body, half, steps, block, sizes, row0),
        grid_spec=pltpu.PrefetchScalarGridSpec(
            num_scalar_prefetch=1, grid=(steps,),
            in_specs=o_specs + o_specs + [
                pl.BlockSpec((width, block), lambda j, s: (0, j)),
                pl.BlockSpec((half, block), lambda j, s: (0, j)),
                pl.BlockSpec((half, block), lambda j, s: (0, j)),
                pl.BlockSpec(memory_space=pl.ANY),
                pl.BlockSpec((1, model), lambda j, s: (0, 0))] + [pl.BlockSpec(memory_space=pl.ANY)] * len(extra),
            out_specs=pl.BlockSpec(memory_space=pl.ANY),
            scratch_shapes=[pltpu.VMEM((tokens, width), jnp.bfloat16), pltpu.VMEM((tokens, width), jnp.bfloat16),
                            pltpu.VMEM((tokens, model), jnp.bfloat16),
                            pltpu.VMEM((steps, tokens, block), jnp.float32), pltpu.VMEM((tokens, 1), jnp.float32),
                            pltpu.SemaphoreType.DMA, pltpu.SemaphoreType.DMA]),
        out_shape=jax.ShapeDtypeStruct(x.shape, jnp.bfloat16),
        input_output_aliases={2 * len(sizes) + 6: 0} if extra else {},
        compiler_params=params(),
        cost_estimate=cost(tokens * 0.045, 4 * width * model),
        name="project",
    )(scalars, *o_list, *ro_list, w_own, w_near, w_far, x, gain, *extra)


def solution(mesh):
    tp_size = mesh.shape['tp']
    OTHER_CHIP = [(0, 2), (2, 0), (1, 3), (3, 1)]
    OTHER_CORE = [(0, 1), (1, 0), (2, 3), (3, 2)]
    OTHER_HALF = [(0, 1), (1, 0)]

    def local_step(x_chunk, w_query, w_key, w_value, w_out, q_gain, k_gain, post_gain, cache_k, cache_v, prefix_len):
        rows, chunk, model = x_chunk.shape
        n_heads = cache_k.shape[2]
        width = n_heads * HD
        total_width = width * tp_size
        cp = lax.axis_index('cp')
        tp = lax.axis_index('tp')
        core = cp % 2
        tokens = x_chunk.reshape(rows * chunk, model)
        scalars = jnp.concatenate([cp[None], prefix_len]).astype(jnp.int32)
        places = jnp.stack([cp, tp]).astype(jnp.int32)
        positions = prefix_len[:, None] + cp * chunk + jnp.arange(chunk, dtype=jnp.int32)[None, :]
        inv_freq = ROPE_BASE ** (-(jnp.arange(HD // 2, dtype=jnp.float32) * 2.0 / HD))
        angles = positions.astype(jnp.float32).reshape(-1, 1) * inv_freq[None, :]
        cos_h, sin_h = jnp.cos(angles), jnp.sin(angles)
        cos = jnp.concatenate([cos_h, cos_h], axis=-1)
        sin = jnp.concatenate([-sin_h, sin_h], axis=-1)
        qg = q_gain.astype(jnp.float32)[None]
        kg = k_gain.astype(jnp.float32)[None]
        pg = post_gain[None]

        def after(value, done):
            return lax.optimization_barrier((value, done))[0]

        def swap_sums(raw):
            own = jnp.sum(raw * raw, axis=-1)[None]
            return own, lax.ppermute(own, 'tp', OTHER_HALF)

        def w_slice(lo, size, done):
            return lax.dynamic_slice_in_dim(after(w_out, done), core * (width // 2) + lo, size, axis=0)

        def rotated(raw, sums, gain, row0, count, raw_row0, done):
            return rope(raw, *sums, after(gain, done), cos, sin, row0, total_width, count, raw_row0)

        def spread(q, r):
            q = q.reshape(r, chunk, width)
            q_chip = lax.ppermute(q, 'cp', OTHER_CHIP)
            q_core = lax.ppermute(q, 'cp', OTHER_CORE)
            return q, q_chip, q_core, lax.ppermute(q_chip, 'cp', OTHER_CORE)

        f32 = jnp.float32
        starts = [sum(GROUPS[:g]) for g in range(len(GROUPS))]
        last_group = len(GROUPS) - 1
        cut = GROUPS[0] * chunk
        raw0 = jnp.dot(tokens[:cut], w_query, preferred_element_type=f32)
        sums0 = swap_sums(raw0)
        ws0 = w_slice(0, 128, raw0)
        ws1 = w_slice(128, 128, raw0)
        q0 = rotated(raw0, sums0, qg, 0, cut, 0, ws1)
        q_sets = [spread(q0, GROUPS[0])]
        wn0 = lax.ppermute(after(ws0, sums0[1]), 'tp', OTHER_HALF)
        raw1 = jnp.dot(after(tokens, q0), w_query, preferred_element_type=f32)
        sums1 = swap_sums(raw1)
        ws2 = w_slice(256, width // 2 - 256, raw1)
        last = ws2
        for g in range(1, len(GROUPS)):
            last = rotated(raw1, sums1, qg, starts[g] * chunk, GROUPS[g] * chunk, 0, last)
            q_sets.append(spread(last, GROUPS[g]))
        wn1 = lax.ppermute(after(ws1, sums1[1]), 'tp', OTHER_HALF)
        k_raw = jnp.dot(after(tokens, last), w_key, preferred_element_type=f32)
        k_sums = swap_sums(k_raw)
        v_flat = jnp.dot(after(tokens, k_sums[0]), w_value, preferred_element_type=f32).astype(jnp.bfloat16)
        k_flat = rotated(k_raw, k_sums, kg, 0, rows * chunk, 0, v_flat)
        wn2 = lax.ppermute(after(ws2, k_sums[1]), 'tp', OTHER_HALF)
        k_new = k_flat.reshape(rows, chunk, width)
        v_new = v_flat.reshape(rows, chunk, width)

        parts = []
        last = k_flat
        merged = []

        def do_merge(g, done):
            keep, _, stat, got, gstat = parts[g]
            send, sstat = merge(keep, got, after(stat, done), gstat, n_heads)
            merged.append((lax.ppermute(send, 'cp', OTHER_CHIP), lax.ppermute(sstat, 'cp', OTHER_CHIP)))
            return sstat

        for g in range(len(GROUPS)):
            keep, give, stat = attention(after(scalars, last), q_sets[g], cache_k, cache_v, k_new, v_new, starts[g])
            parts.append((keep, give, stat, lax.ppermute(give, 'cp', OTHER_CORE), lax.ppermute(stat, 'cp', OTHER_CORE)))
            last = stat
            if g >= 1:
                last = do_merge(g - 1, last)
        last = do_merge(last_group, last)
        w_near = jnp.concatenate([after(wn0, last), wn1, wn2], axis=0)
        w_far = lax.ppermute(w_near, 'cp', OTHER_CORE)
        last = w_near

        block_out = None
        g = 0
        for count in P_GROUPS:
            o_list, ro_list = [], []
            first_row = starts[g]
            for _ in range(count):
                keep, give, stat, got, gstat = parts[g]
                far, fstat = merged[g]
                o = finish(keep, got, far, after(stat, last), gstat, fstat, n_heads).reshape(GROUPS[g] * chunk, width)
                o_list.append(o)
                ro_list.append(lax.ppermute(o, 'tp', OTHER_HALF))
                last = o
                g += 1
            block_out = project(after(places, last), o_list, ro_list, w_out, w_near, w_far, tokens, pg, first_row * chunk, block_out)
            last = block_out
        block_out = block_out.reshape(rows, chunk, model)
        shape = (rows, chunk, n_heads, HD)
        return block_out, k_new.reshape(shape), v_new.reshape(shape)

    x_spec = P('dp', 'cp', None)
    head_spec = P('dp', 'cp', 'tp', None)
    in_specs = (x_spec, P(None, 'tp'), P(None, 'tp'), P(None, 'tp'), P('tp', None), P('tp'), P('tp'), P(None), head_spec, head_spec, P('dp'))
    out_specs = (x_spec, head_spec, head_spec)

    return jax.shard_map(local_step, mesh=mesh, in_specs=in_specs, out_specs=out_specs, check_vma=False)
```

```python
import functools

import jax
import jax.numpy as jnp
from jax import lax
from jax.experimental import pallas as pl
from jax.experimental.pallas import tpu as pltpu
from jax.sharding import PartitionSpec as P

NORM_EPS = 1e-6
ROPE_BASE = 500000.0
NEG = -1e30
FLOOR = -5e29
LOG2E = 1.4426950408889634
HD = 128
LAG = 1
ROPE_BLOCK = 256
P_BLOCK = 512
GROUPS = ((24, 8), (0, 8), (8, 8), (16, 4), (20, 4))
P_GROUPS = ((0, 1), (2, 3, 4))
PIECES = (256, 768)
VMEM_LIMIT = 60 * 1024 * 1024


def cost(micros, moved):
    return pl.CostEstimate(flops=int(micros * 9e8), bytes_accessed=moved, transcendentals=0)


def params():
    return pltpu.CompilerParams(dimension_semantics=("arbitrary",), vmem_limit_bytes=VMEM_LIMIT)


def dense_body(steps, x, w, out, sums, acc):
    j = pl.program_id(0)
    r = jnp.dot(x[...], w[...], preferred_element_type=jnp.float32)
    out[...] = r
    sq = r * r
    part = sq[:, :HD]
    for c in range(HD, sq.shape[1], HD):
        part = part + sq[:, c:c + HD]
    acc[...] = jnp.where(j == 0, part, acc[...] + part)

    @pl.when(j == steps - 1)
    def _():
        for t in range(0, acc.shape[0], HD):
            sums[:, t:t + HD] = jnp.sum(acc[t:t + HD, :].T, axis=0, keepdims=True)


def dense(x, w, row0, tokens):
    model, width = w.shape
    block = 512
    steps = width // block
    row_block = row0 // tokens
    return pl.pallas_call(
        functools.partial(dense_body, steps),
        grid=(steps,),
        in_specs=[pl.BlockSpec((tokens, model), lambda j: (row_block, 0), pipeline_mode=pl.Buffered(1)),
                  pl.BlockSpec((model, block), lambda j: (0, j))],
        out_specs=[pl.BlockSpec((tokens, block), lambda j: (0, j)), pl.BlockSpec((1, tokens), lambda j: (0, 0))],
        out_shape=[jax.ShapeDtypeStruct((tokens, width), jnp.float32), jax.ShapeDtypeStruct((1, tokens), jnp.float32)],
        scratch_shapes=[pltpu.VMEM((tokens, HD), jnp.float32)],
        compiler_params=params(),
        cost_estimate=cost(8 + tokens * 0.015, model * width * 2),
        name="dense",
    )(x, w)


def rope_body(total_width, n_heads, raw, own, peer, gain, cos, sin, out):
    inv = lax.rsqrt((own[...] + peer[...]) / total_width + NORM_EPS)
    inv = jnp.concatenate([jnp.broadcast_to(inv[:, i:i + HD], (HD, HD)).T for i in range(0, inv.shape[1], HD)], axis=0)
    cos_t = cos[...]
    sin_t = sin[...]
    for h in range(n_heads):
        cols = slice(h * HD, (h + 1) * HD)
        u = raw[:, cols] * inv * gain[:, cols]
        out[:, cols] = (u * cos_t + pltpu.roll(u, HD // 2, 1) * sin_t).astype(jnp.bfloat16)


def rope(raw, own, peer, gain, cos, sin, row0, total_width, tokens, raw_row0):
    width = raw.shape[1]
    block = ROPE_BLOCK if tokens % ROPE_BLOCK == 0 else 128
    base = row0 // block
    off = (row0 - raw_row0) // block
    return pl.pallas_call(
        functools.partial(rope_body, total_width, width // HD),
        grid=(tokens // block,),
        in_specs=[pl.BlockSpec((block, width), lambda i: (i + off, 0)),
                  pl.BlockSpec((1, block), lambda i: (0, i + off)),
                  pl.BlockSpec((1, block), lambda i: (0, i + off)),
                  pl.BlockSpec((1, width), lambda i: (0, 0)),
                  pl.BlockSpec((block, HD), lambda i: (i + base, 0)),
                  pl.BlockSpec((block, HD), lambda i: (i + base, 0))],
        out_specs=pl.BlockSpec((block, width), lambda i: (i, 0)),
        out_shape=jax.ShapeDtypeStruct((tokens, width), jnp.bfloat16),
        compiler_params=params(),
        cost_estimate=cost(tokens * 0.005, tokens * width * 6),
        name="rope",
    )(raw, own, peer, gain, cos, sin)


def attn_body(n_heads, row0, chunk, slots, pitch, sc_ref, qa, qb, qc, qd, ck, cv, kc, vc, keep, give, stat, ks, vs):
    b = pl.program_id(0)
    cp = sc_ref[0]
    valid_len = sc_ref[1 + row0 + b]
    tokens = 4 * chunk
    keys = slots + chunk
    for t in range(slots):
        ks[t * pitch:t * pitch + n_heads, :] = ck[0, t].astype(jnp.float32)
        vs[t * pitch:t * pitch + n_heads, :] = cv[0, t].astype(jnp.float32)
    row = lax.broadcasted_iota(jnp.int32, (keys, tokens), 0)
    col = lax.broadcasted_iota(jnp.int32, (keys, tokens), 1)
    part = col // chunk
    rel = jnp.where(part == 1, 2, jnp.where(part == 2, 1, part))
    query = jnp.bitwise_xor(rel, cp) * chunk + col % chunk
    chunk_key = cp * chunk + row - slots
    ok = jnp.where(row < slots, row + cp * slots - valid_len, chunk_key - query - 1) < 0
    scale = HD ** -0.5 * LOG2E
    contract_last = (((1,), (1,)), ((), ()))
    contract_first = (((0,), (0,)), ((), ()))

    def cols(h):
        return slice(h * HD, (h + 1) * HD)

    def scores(h):
        q = jnp.concatenate([qa[0, :, cols(h)], qb[0, :, cols(h)], qc[0, :, cols(h)], qd[0, :, cols(h)]], axis=0)
        k = jnp.concatenate([ks[pl.ds(h, slots, stride=pitch), :].astype(jnp.bfloat16), kc[0, :, cols(h)]], axis=0)
        return lax.dot_general(k, q, contract_last, preferred_element_type=jnp.float32)

    def soft(h, s):
        s = jnp.where(ok, s * scale, NEG)
        top = jnp.maximum(jnp.max(s, axis=0, keepdims=True), FLOOR)
        p = jnp.exp2(s - top)
        stat[0, h:h + 1, :] = top
        stat[0, n_heads + h:n_heads + h + 1, :] = jnp.sum(p, axis=0, keepdims=True)
        return p.astype(jnp.bfloat16)

    def values(h, p):
        v = jnp.concatenate([vs[pl.ds(h, slots, stride=pitch), :].astype(jnp.bfloat16), vc[0, :, cols(h)]], axis=0)
        num = lax.dot_general(p, v, contract_first, preferred_element_type=jnp.float32)
        keep[0, :, cols(h)] = num[:2 * chunk]
        give[0, :, cols(h)] = num[2 * chunk:]

    s_live, p_live = {}, {}
    for step in range(n_heads + 2 * LAG):
        if step < n_heads:
            s_live[step] = scores(step)
        h = step - LAG
        if 0 <= h < n_heads:
            p_live[h] = soft(h, s_live.pop(h))
        h = step - 2 * LAG
        if 0 <= h < n_heads:
            values(h, p_live.pop(h))


def attention(scalars, q_parts, cache_k, cache_v, k_new, k_row, v_new, v_row, row0):
    rows, chunk, width = q_parts[0].shape
    _, slots, n_heads, _ = cache_k.shape
    pitch = n_heads + 8
    q_spec = pl.BlockSpec((1, chunk, width), lambda b, s: (b, 0, 0))
    k_spec = pl.BlockSpec((1, chunk, width), lambda b, s: (b + k_row, 0, 0))
    v_spec = pl.BlockSpec((1, chunk, width), lambda b, s: (b + v_row, 0, 0))
    cache_spec = pl.BlockSpec((1, slots, n_heads, HD), lambda b, s: (b + row0, 0, 0, 0))
    out_spec = pl.BlockSpec((1, 2 * chunk, width), lambda b, s: (b, 0, 0))
    stat_spec = pl.BlockSpec((1, 2 * n_heads, 4 * chunk), lambda b, s: (b, 0, 0))
    out = jax.ShapeDtypeStruct((rows, 2 * chunk, width), jnp.float32)
    return pl.pallas_call(
        functools.partial(attn_body, n_heads, row0, chunk, slots, pitch),
        grid_spec=pltpu.PrefetchScalarGridSpec(
            num_scalar_prefetch=1, grid=(rows,),
            in_specs=[q_spec] * 4 + [cache_spec] * 2 + [k_spec, v_spec],
            out_specs=[out_spec] * 2 + [stat_spec],
            scratch_shapes=[pltpu.VMEM((slots * pitch, HD), jnp.float32)] * 2),
        out_shape=[out, out, jax.ShapeDtypeStruct((rows, 2 * n_heads, 4 * chunk), jnp.float32)],
        compiler_params=params(),
        cost_estimate=cost(rows * 3.9, rows * slots * width * 6),
        name="attention",
    )(scalars, *q_parts, cache_k, cache_v, k_new, v_new)


def pack_rows(stats, span, chunk, shift):
    lane = lax.broadcasted_iota(jnp.int32, stats[0].shape, 1) // chunk
    width = stats[0].shape[1]
    packed = stats[0] if shift == 0 else pltpu.roll(stats[0], (-shift * chunk) % width, 1)
    for i in range(1, span):
        step = ((i - shift) * chunk) % width
        packed = jnp.where(lane == i, pltpu.roll(stats[i], step, 1) if step else stats[i], packed)
    return packed


def merge_body(n_heads, chunk, span, keep, got, stat, gstat, out, ostat):
    mine = pack_rows([stat[i] for i in range(span)], span, chunk, 1)
    theirs = pack_rows([gstat[i] for i in range(span)], span, chunk, 3)
    t0, d0, t1, d1 = mine[:n_heads], mine[n_heads:], theirs[:n_heads], theirs[n_heads:]
    top = jnp.maximum(t0, t1)
    w0 = jnp.exp2(t0 - top)
    w1 = jnp.exp2(t1 - top)
    ostat[0] = jnp.concatenate([top, w0 * d0 + w1 * d1], axis=0)
    w = jnp.concatenate([w0, w1], axis=0).T
    tokens = span * chunk
    for h in range(n_heads):
        cols = slice(h * HD, (h + 1) * HD)
        val = keep[:, :, cols].reshape(tokens, HD) * w[:, h:h + 1]
        val = val + got[:, :, cols].reshape(tokens, HD) * w[:, n_heads + h:n_heads + h + 1]
        out[:, :, cols] = val.reshape(span, chunk, HD)


def merge(keep, got, stat, gstat, n_heads):
    rows, chunk2, width = keep.shape
    chunk = chunk2 // 2
    span = 4
    half = pl.BlockSpec((span, chunk, width), lambda i: (i, 1, 0))
    stats = pl.BlockSpec((span, 2 * n_heads, 4 * chunk), lambda i: (i, 0, 0))
    return pl.pallas_call(
        functools.partial(merge_body, n_heads, chunk, span),
        grid=(rows // span,),
        in_specs=[half, half, stats, stats],
        out_specs=[pl.BlockSpec((span, chunk, width), lambda i: (i, 0, 0)),
                   pl.BlockSpec((1, 2 * n_heads, 4 * chunk), lambda i: (i, 0, 0))],
        out_shape=[jax.ShapeDtypeStruct((rows, chunk, width), jnp.float32),
                   jax.ShapeDtypeStruct((rows // span, 2 * n_heads, 4 * chunk), jnp.float32)],
        compiler_params=params(),
        cost_estimate=cost(rows * 0.3, rows * chunk * width * 12),
        name="merge",
    )(keep, got, stat, gstat)


def finish_body(n_heads, chunk, span, keep, got, far, stat, gstat, fstat, out):
    sets = [pack_rows([stat[i] for i in range(span)], span, chunk, 0),
            pack_rows([gstat[i] for i in range(span)], span, chunk, 2), fstat[0]]
    pairs = [(x[:n_heads], x[n_heads:]) for x in sets]
    top = jnp.maximum(jnp.maximum(pairs[0][0], pairs[1][0]), pairs[2][0])
    ws = [jnp.exp2(t - top) for t, _ in pairs]
    den = ws[0] * pairs[0][1] + ws[1] * pairs[1][1] + ws[2] * pairs[2][1]
    inv = 1.0 / den
    w = jnp.concatenate([x * inv for x in ws], axis=0).T
    tokens = span * chunk
    for h in range(n_heads):
        cols = slice(h * HD, (h + 1) * HD)
        val = keep[:, :, cols].reshape(tokens, HD) * w[:, h:h + 1]
        val = val + got[:, :, cols].reshape(tokens, HD) * w[:, n_heads + h:n_heads + h + 1]
        val = val + far[:, :, cols].reshape(tokens, HD) * w[:, 2 * n_heads + h:2 * n_heads + h + 1]
        out[:, :, cols] = val.astype(jnp.bfloat16).reshape(span, chunk, HD)


def finish(keep, got, far, stat, gstat, fstat, n_heads):
    rows, chunk2, width = keep.shape
    chunk = chunk2 // 2
    span = 4
    half = pl.BlockSpec((span, chunk, width), lambda i: (i, 0, 0))
    stats = pl.BlockSpec((span, 2 * n_heads, 4 * chunk), lambda i: (i, 0, 0))
    return pl.pallas_call(
        functools.partial(finish_body, n_heads, chunk, span),
        grid=(rows // span,),
        in_specs=[half, half, half, stats, stats, pl.BlockSpec((1, 2 * n_heads, 4 * chunk), lambda i: (i, 0, 0))],
        out_specs=half,
        out_shape=jax.ShapeDtypeStruct((rows, chunk, width), jnp.bfloat16),
        compiler_params=params(),
        cost_estimate=cost(rows * 0.4, rows * chunk * width * 14),
        name="finish",
    )(keep, got, far, stat, gstat, fstat)


def chain(o, steps):
    total = None
    for at, part in steps:
        term = jnp.dot(o[:, pl.ds(at, part.shape[0])], part[...], preferred_element_type=jnp.float32)
        total = term if total is None else total + term
    return total


def own_steps(w_own, core, half):
    steps = []
    for side in (core, 1 - core):
        at = 0
        for size in PIECES:
            lo = pl.multiple_of(side * half + at, HD)
            steps.append((lo, w_own.at[pl.ds(lo, size)]))
            at += size
    return steps


def peer_steps(near, far, core, half):
    steps = []
    for side, parts in ((core, near), (1 - core, far)):
        at = 0
        for size, part in zip(PIECES, parts):
            steps.append((pl.multiple_of(side * half + at, HD), part))
            at += size
    return steps


def gather_rows(dst, pieces):
    at = 0
    for piece in pieces:
        size = piece.shape[0]
        dst[at:at + size, :] = piece[...]
        at += size


def own_body(n, half, sc_ref, *refs):
    o_in = refs[:n]
    w_own, out, o = refs[n:]
    core = sc_ref[0] % 2

    @pl.when(pl.program_id(0) == 0)
    def _():
        gather_rows(o, o_in)

    out[...] = chain(o, own_steps(w_own, core, half))


def project_body(n, half, steps, block, row_starts, sc_ref, *refs):
    p = len(PIECES)
    j = pl.program_id(0)
    core = sc_ref[0] % 2
    ro_in, refs = refs[:n], refs[n:]
    near, far, refs = refs[:p], refs[p:2 * p], refs[2 * p:]
    x_hbm, gain, ready = refs[:3]
    out_hbm, ro, x, acc, ssq, sem, out_sem = refs[-7:]
    sizes = [r.shape[0] for r in ro_in]
    spots = [sum(sizes[:k]) for k in range(n)]

    def copies(out):
        made = []
        for k in range(n):
            there = pl.ds(row_starts[k], sizes[k])
            here = x.at[pl.ds(spots[k], sizes[k])]
            if out:
                made.append(pltpu.make_async_copy(here, out_hbm.at[there], out_sem.at[k]))
            else:
                made.append(pltpu.make_async_copy(x_hbm.at[there], here, sem.at[k]))
        return made

    @pl.when(j == 0)
    def _():
        for c in copies(False):
            c.start()
        gather_rows(ro, ro_in)

    a = ready[...] + chain(ro, peer_steps(near, far, core, half))
    acc[j] = a
    sq = jnp.sum(a * a, axis=-1, keepdims=True)
    ssq[...] = jnp.where(j == 0, sq, ssq[...] + sq)

    @pl.when(j == steps - 1)
    def _():
        for c in copies(False):
            c.wait()
        inv = lax.rsqrt(ssq[...] / (steps * block) + NORM_EPS)
        for k in range(steps):
            cols = slice(k * block, (k + 1) * block)
            y = x[:, cols].astype(jnp.float32) + acc[k] * inv * gain[:, cols].astype(jnp.float32)
            x[:, cols] = y.astype(jnp.bfloat16)
        for c in copies(True):
            c.start()
        for c in copies(True):
            c.wait()


def rows_spec(pieces):
    return [pl.BlockSpec(o.shape, lambda j, s: (0, 0), pipeline_mode=pl.Buffered(1)) for o in pieces]


def project_own(scalars, o_list, w_own):
    tokens, width = sum(o.shape[0] for o in o_list), o_list[0].shape[1]
    model = w_own.shape[1]
    block = P_BLOCK
    return pl.pallas_call(
        functools.partial(own_body, len(o_list), width // 2),
        grid_spec=pltpu.PrefetchScalarGridSpec(
            num_scalar_prefetch=1, grid=(model // block,),
            in_specs=rows_spec(o_list) + [pl.BlockSpec((width, block), lambda j, s: (0, j))],
            out_specs=pl.BlockSpec((tokens, block), lambda j, s: (0, j)),
            scratch_shapes=[pltpu.VMEM((tokens, width), jnp.bfloat16)]),
        out_shape=jax.ShapeDtypeStruct((tokens, model), jnp.float32),
        compiler_params=params(),
        cost_estimate=cost(6 + tokens * 0.02, 2 * width * model),
        name="project_own",
    )(scalars, *o_list, w_own)


def project(scalars, ready, ro_list, near, far, x, gain, row_starts, so_far):
    n = len(ro_list)
    tokens, width = sum(o.shape[0] for o in ro_list), ro_list[0].shape[1]
    model = x.shape[1]
    block = P_BLOCK
    steps = model // block
    anywhere = pl.BlockSpec(memory_space=pl.ANY)
    w_specs = [pl.BlockSpec((p.shape[0], block), lambda j, s: (0, j)) for p in list(near) + list(far)]
    specs = rows_spec(ro_list) + w_specs + [anywhere, pl.BlockSpec((1, model), lambda j, s: (0, 0)),
                                            pl.BlockSpec((tokens, block), lambda j, s: (0, j))]
    args = [*ro_list, *near, *far, x, gain, ready]
    alias = {}
    if so_far is not None:
        alias = {1 + len(args): 0}
        specs.append(anywhere)
        args.append(so_far)
    return pl.pallas_call(
        functools.partial(project_body, n, width // 2, steps, block, row_starts),
        grid_spec=pltpu.PrefetchScalarGridSpec(
            num_scalar_prefetch=1, grid=(steps,), in_specs=specs, out_specs=anywhere,
            scratch_shapes=[pltpu.VMEM((tokens, width), jnp.bfloat16), pltpu.VMEM((tokens, model), jnp.bfloat16),
                            pltpu.VMEM((steps, tokens, block), jnp.float32), pltpu.VMEM((tokens, 1), jnp.float32),
                            pltpu.SemaphoreType.DMA((n,)), pltpu.SemaphoreType.DMA((n,))]),
        out_shape=jax.ShapeDtypeStruct(x.shape, jnp.bfloat16),
        input_output_aliases=alias,
        compiler_params=params(),
        cost_estimate=cost(10 + tokens * 0.02, 2 * width * model),
        name="project",
    )(scalars, *args)


def solution(mesh):
    tp_size = mesh.shape['tp']
    OTHER_CHIP = [(0, 2), (2, 0), (1, 3), (3, 1)]
    OTHER_CORE = [(0, 1), (1, 0), (2, 3), (3, 2)]
    OTHER_HALF = [(0, 1), (1, 0)]

    def local_step(x_chunk, w_query, w_key, w_value, w_out, q_gain, k_gain, post_gain, cache_k, cache_v, prefix_len):
        rows, chunk, model = x_chunk.shape
        n_heads = cache_k.shape[2]
        width = n_heads * HD
        total_width = width * tp_size
        cp = lax.axis_index('cp')
        tp = lax.axis_index('tp')
        core = cp % 2
        tokens = x_chunk.reshape(rows * chunk, model)
        scalars = jnp.concatenate([cp[None], prefix_len]).astype(jnp.int32)
        places = jnp.stack([cp, tp]).astype(jnp.int32)
        positions = prefix_len[:, None] + cp * chunk + jnp.arange(chunk, dtype=jnp.int32)[None, :]
        inv_freq = ROPE_BASE ** (-(jnp.arange(HD // 2, dtype=jnp.float32) * 2.0 / HD))
        angles = positions.astype(jnp.float32).reshape(-1, 1) * inv_freq[None, :]
        cos_h, sin_h = jnp.cos(angles), jnp.sin(angles)
        cos = jnp.concatenate([cos_h, cos_h], axis=-1)
        sin = jnp.concatenate([-sin_h, sin_h], axis=-1)
        qg = q_gain.astype(jnp.float32)[None]
        kg = k_gain.astype(jnp.float32)[None]
        pg = post_gain[None]

        def after(value, done):
            return lax.optimization_barrier((value, done))[0]

        def swap(own):
            return own, lax.ppermute(own, 'tp', OTHER_HALF)

        def w_slice(n, done):
            lo = core * (width // 2) + sum(PIECES[:n])
            return lax.dynamic_slice_in_dim(after(w_out, done), lo, PIECES[n], axis=0)

        def rotated(raw, sums, gain, row0, count, raw_row0, done):
            return rope(raw, *sums, after(gain, done), cos, sin, row0 * chunk, total_width, count * chunk, raw_row0 * chunk)

        def spread(q):
            q = q.reshape(-1, chunk, width)
            q_chip = lax.ppermute(q, 'cp', OTHER_CHIP)
            q_core = lax.ppermute(q, 'cp', OTHER_CORE)
            return q, q_chip, q_core, lax.ppermute(q_chip, 'cp', OTHER_CORE)

        f32 = jnp.float32
        split, first_rows = GROUPS[0]
        raw0, own0 = dense(tokens, w_query, split * chunk, first_rows * chunk)
        sums0 = swap(own0)
        ws0 = w_slice(0, own0)
        q0 = rotated(raw0, sums0, qg, split, first_rows, split, ws0)
        q_sets = [spread(q0)]
        raw1, own1 = dense(after(tokens, q0), w_query, 0, split * chunk)
        sums1 = swap(own1)
        ws1 = w_slice(1, own1)
        last = ws1
        for g in range(1, len(GROUPS)):
            last = rotated(raw1, sums1, qg, *GROUPS[g], 0, last)
            q_sets.append(spread(last))
        wn0 = lax.ppermute(after(ws0, own1), 'tp', OTHER_HALF)
        k_raw = jnp.dot(after(tokens, last), w_key, preferred_element_type=f32)
        k_sums = swap(jnp.sum(k_raw * k_raw, axis=-1)[None])
        v_flat = jnp.dot(after(tokens, k_sums[0]), w_value, preferred_element_type=f32).astype(jnp.bfloat16)
        k_first = rotated(k_raw, k_sums, kg, split, first_rows, 0, v_flat)
        wn1 = lax.ppermute(after(ws1, k_sums[0]), 'tp', OTHER_HALF)
        near = (wn0, wn1)
        far_w = tuple(lax.ppermute(w, 'cp', OTHER_CORE) for w in near)
        v_new = v_flat.reshape(rows, chunk, width)
        k_new = [(k_first.reshape(-1, chunk, width), 0)]

        parts, merged, o_mine, o_peer = {}, {}, {}, {}

        def attend(g, done):
            row0 = GROUPS[g][0]
            ks, _ = k_new[min(g, 1)]
            keep, give, stat = attention(after(scalars, done), q_sets[g], cache_k, cache_v,
                                      ks, row0 if g else 0, v_new, row0, row0)
            parts[g] = (keep, give, stat, lax.ppermute(give, 'cp', OTHER_CORE), lax.ppermute(stat, 'cp', OTHER_CORE))
            return stat

        def combine(g, done):
            keep, _, stat, got, gstat = parts[g]
            send, sstat = merge(keep, got, after(stat, done), gstat, n_heads)
            merged[g] = (lax.ppermute(send, 'cp', OTHER_CHIP), lax.ppermute(sstat, 'cp', OTHER_CHIP))
            return sstat

        def close(g, done):
            keep, _, stat, got, gstat = parts[g]
            o = finish(keep, got, merged[g][0], after(stat, done), gstat, merged[g][1], n_heads)
            o_mine[g] = o.reshape(-1, width)
            o_peer[g] = lax.ppermute(o_mine[g], 'tp', OTHER_HALF)
            return o

        def mix(n, ready, so_far=None):
            groups = P_GROUPS[n]
            return project(places, ready, [o_peer[g] for g in groups],
                          near, far_w, tokens, pg, tuple(GROUPS[g][0] * chunk for g in groups), so_far)

        def own_part(n, done):
            return project_own(after(places, done), [o_mine[g] for g in P_GROUPS[n]], w_out)

        shape = (rows, chunk, n_heads, HD)
        last = attend(0, k_first)
        k_rest = rotated(k_raw, k_sums, kg, 0, split, 0, last)
        k_new.append((k_rest.reshape(-1, chunk, width), 0))
        last = combine(0, k_rest)
        last = attend(1, last)
        last = attend(2, last)
        last = combine(1, last)
        last = close(0, last)
        last = attend(3, last)
        last = combine(2, last)
        last = attend(4, last)
        last = combine(3, last)
        last = combine(4, last)
        last = close(1, last)
        block_out = mix(0, own_part(0, last))
        last = close(2, block_out)
        last = close(3, last)
        chunk_k = jnp.concatenate([after(k_rest, last), k_first], axis=0).reshape(shape)
        chunk_v = after(v_flat, last).reshape(shape)
        last = close(4, (chunk_k, chunk_v))
        block_out = mix(1, own_part(1, last), block_out)
        return block_out.reshape(rows, chunk, model), chunk_k, chunk_v

    x_spec = P('dp', 'cp', None)
    head_spec = P('dp', 'cp', 'tp', None)
    in_specs = (x_spec, P(None, 'tp'), P(None, 'tp'), P(None, 'tp'), P('tp', None), P('tp'), P('tp'), P(None), head_spec, head_spec, P('dp'))
    out_specs = (x_spec, head_spec, head_spec)

    return jax.shard_map(local_step, mesh=mesh, in_specs=in_specs, out_specs=out_specs, check_vma=False)
```

```python
import functools

import jax
import jax.numpy as jnp
from jax import lax
from jax.experimental import pallas as pl
from jax.experimental.pallas import tpu as pltpu
from jax.sharding import PartitionSpec as P

NORM_EPS = 1e-6
ROPE_BASE = 500000.0
NEG = -1e30
FLOOR = -5e29
LOG2E = 1.4426950408889634
HD = 128
LAG = 2
ROPE_BLOCK = 256
P_BLOCK = 1024
GROUPS = ((24, 8), (0, 8), (8, 8), (16, 8))
ATTEND = ((0, 0, 4), (0, 4, 4), (1, 0, 8), (2, 0, 8), (3, 0, 8))
MERGE = ((0, 0, 4), (1, 0, 4), (2, 0, 8), (3, 0, 8), (4, 0, 4), (4, 4, 4))
P_GROUPS = ((0, 1, 2), (3, 4, 5))
PIECES = (256, 768)
VMEM_LIMIT = 60 * 1024 * 1024


def cost(micros, moved):
    return pl.CostEstimate(flops=int(micros * 9e8), bytes_accessed=moved, transcendentals=0)


def params():
    return pltpu.CompilerParams(dimension_semantics=("arbitrary",), vmem_limit_bytes=VMEM_LIMIT)


def dense_body(steps, x, w, out, sums, acc):
    j = pl.program_id(0)
    r = jnp.dot(x[...], w[...], preferred_element_type=jnp.float32)
    out[...] = r.astype(out.dtype)
    sq = r * r
    part = sq[:, :HD]
    for c in range(HD, sq.shape[1], HD):
        part = part + sq[:, c:c + HD]
    acc[...] = jnp.where(j == 0, part, acc[...] + part)

    @pl.when(j == steps - 1)
    def _():
        for t in range(0, acc.shape[0], HD):
            sums[:, t:t + HD] = jnp.sum(acc[t:t + HD, :].T, axis=0, keepdims=True)


def dense(x, w, row0, tokens, dtype=jnp.float32):
    model, width = w.shape
    block = 512
    steps = width // block
    row_block = row0 // tokens
    return pl.pallas_call(
        functools.partial(dense_body, steps),
        grid=(steps,),
        in_specs=[pl.BlockSpec((tokens, model), lambda j: (row_block, 0), pipeline_mode=pl.Buffered(1)),
                  pl.BlockSpec((model, block), lambda j: (0, j))],
        out_specs=[pl.BlockSpec((tokens, block), lambda j: (0, j)), pl.BlockSpec((1, tokens), lambda j: (0, 0))],
        out_shape=[jax.ShapeDtypeStruct((tokens, width), dtype), jax.ShapeDtypeStruct((1, tokens), jnp.float32)],
        scratch_shapes=[pltpu.VMEM((tokens, HD), jnp.float32)],
        compiler_params=params(),
        cost_estimate=cost(8 + tokens * 0.015, model * width * 2),
        name="dense",
    )(x, w)


def rope_body(total_width, n_heads, raw, own, peer, gain, cos, sin, out):
    inv = lax.rsqrt((own[...] + peer[...]) / total_width + NORM_EPS)
    inv = jnp.concatenate([jnp.broadcast_to(inv[:, i:i + HD], (HD, HD)).T for i in range(0, inv.shape[1], HD)], axis=0)
    cos_t = cos[...]
    sin_t = sin[...]
    for h in range(n_heads):
        cols = slice(h * HD, (h + 1) * HD)
        u = raw[:, cols] * inv * gain[:, cols]
        out[:, cols] = (u * cos_t + pltpu.roll(u, HD // 2, 1) * sin_t).astype(jnp.bfloat16)


def rope(raw, own, peer, gain, cos, sin, row0, total_width, tokens, raw_row0):
    width = raw.shape[1]
    block = ROPE_BLOCK if tokens % ROPE_BLOCK == 0 else 128
    base = row0 // block
    off = (row0 - raw_row0) // block
    return pl.pallas_call(
        functools.partial(rope_body, total_width, width // HD),
        grid=(tokens // block,),
        in_specs=[pl.BlockSpec((block, width), lambda i: (i + off, 0)),
                  pl.BlockSpec((1, block), lambda i: (0, i + off)),
                  pl.BlockSpec((1, block), lambda i: (0, i + off)),
                  pl.BlockSpec((1, width), lambda i: (0, 0)),
                  pl.BlockSpec((block, HD), lambda i: (i + base, 0)),
                  pl.BlockSpec((block, HD), lambda i: (i + base, 0))],
        out_specs=pl.BlockSpec((block, width), lambda i: (i, 0)),
        out_shape=jax.ShapeDtypeStruct((tokens, width), jnp.bfloat16),
        compiler_params=params(),
        cost_estimate=cost(tokens * 0.005, tokens * width * 6),
        name="rope",
    )(raw, own, peer, gain, cos, sin)


def attn_body(n_heads, row0, chunk, slots, pitch, sc_ref, qa, qb, qc, qd, ck, cv, kc, vc, keep, give, stat, ks, vs):
    b = pl.program_id(0)
    cp = sc_ref[0]
    valid_len = sc_ref[1 + row0 + b]
    tokens = 4 * chunk
    keys = slots + chunk
    for t in range(slots):
        ks[t * pitch:t * pitch + n_heads, :] = ck[0, t].astype(jnp.float32)
        vs[t * pitch:t * pitch + n_heads, :] = cv[0, t].astype(jnp.float32)
    row = lax.broadcasted_iota(jnp.int32, (keys, tokens), 0)
    col = lax.broadcasted_iota(jnp.int32, (keys, tokens), 1)
    part = col // chunk
    rel = jnp.where(part == 1, 2, jnp.where(part == 2, 1, part))
    query = jnp.bitwise_xor(rel, cp) * chunk + col % chunk
    chunk_key = cp * chunk + row - slots
    ok = jnp.where(row < slots, row + cp * slots - valid_len, chunk_key - query - 1) < 0
    scale = HD ** -0.5 * LOG2E
    contract_last = (((1,), (1,)), ((), ()))
    contract_first = (((0,), (0,)), ((), ()))

    def cols(h):
        return slice(h * HD, (h + 1) * HD)

    def scores(h):
        q = jnp.concatenate([qa[0, :, cols(h)], qb[0, :, cols(h)], qc[0, :, cols(h)], qd[0, :, cols(h)]], axis=0)
        k = jnp.concatenate([ks[pl.ds(h, slots, stride=pitch), :].astype(jnp.bfloat16), kc[0, :, cols(h)]], axis=0)
        return lax.dot_general(k, q, contract_last, preferred_element_type=jnp.float32)

    def soft(h, s):
        s = jnp.where(ok, s * scale, NEG)
        top = jnp.maximum(jnp.max(s, axis=0, keepdims=True), FLOOR)
        p = jnp.exp2(s - top)
        stat[0, h:h + 1, :] = top
        stat[0, n_heads + h:n_heads + h + 1, :] = jnp.sum(p, axis=0, keepdims=True)
        return p.astype(jnp.bfloat16)

    def values(h, p):
        v = jnp.concatenate([vs[pl.ds(h, slots, stride=pitch), :].astype(jnp.bfloat16), vc[0, :, cols(h)]], axis=0)
        num = lax.dot_general(p, v, contract_first, preferred_element_type=jnp.float32)
        keep[0, :, cols(h)] = num[:2 * chunk]
        give[0, :, cols(h)] = num[2 * chunk:]

    s_live, p_live = {}, {}
    for step in range(n_heads + 2 * LAG):
        if step < n_heads:
            s_live[step] = scores(step)
        h = step - LAG
        if 0 <= h < n_heads:
            p_live[h] = soft(h, s_live.pop(h))
        h = step - 2 * LAG
        if 0 <= h < n_heads:
            values(h, p_live.pop(h))


def attention(scalars, q_parts, q_row, rows, cache_k, cache_v, k_new, k_row, v_new, v_row, row0):
    _, chunk, width = q_parts[0].shape
    _, slots, n_heads, _ = cache_k.shape
    pitch = n_heads + 8
    q_spec = pl.BlockSpec((1, chunk, width), lambda b, s: (b + q_row, 0, 0))
    k_spec = pl.BlockSpec((1, chunk, width), lambda b, s: (b + k_row, 0, 0))
    v_spec = pl.BlockSpec((1, chunk, width), lambda b, s: (b + v_row, 0, 0))
    cache_spec = pl.BlockSpec((1, slots, n_heads, HD), lambda b, s: (b + row0, 0, 0, 0))
    out_spec = pl.BlockSpec((1, 2 * chunk, width), lambda b, s: (b, 0, 0))
    stat_spec = pl.BlockSpec((1, 2 * n_heads, 4 * chunk), lambda b, s: (b, 0, 0))
    out = jax.ShapeDtypeStruct((rows, 2 * chunk, width), jnp.float32)
    return pl.pallas_call(
        functools.partial(attn_body, n_heads, row0, chunk, slots, pitch),
        grid_spec=pltpu.PrefetchScalarGridSpec(
            num_scalar_prefetch=1, grid=(rows,),
            in_specs=[q_spec] * 4 + [cache_spec] * 2 + [k_spec, v_spec],
            out_specs=[out_spec] * 2 + [stat_spec],
            scratch_shapes=[pltpu.VMEM((slots * pitch, HD), jnp.float32)] * 2),
        out_shape=[out, out, jax.ShapeDtypeStruct((rows, 2 * n_heads, 4 * chunk), jnp.float32)],
        compiler_params=params(),
        cost_estimate=cost(rows * 3.9, rows * slots * width * 6),
        name="attention",
    )(scalars, *q_parts, cache_k, cache_v, k_new, v_new)


def pack_rows(stats, span, chunk, shift):
    lane = lax.broadcasted_iota(jnp.int32, stats[0].shape, 1) // chunk
    width = stats[0].shape[1]
    packed = stats[0] if shift == 0 else pltpu.roll(stats[0], (-shift * chunk) % width, 1)
    for i in range(1, span):
        step = ((i - shift) * chunk) % width
        packed = jnp.where(lane == i, pltpu.roll(stats[i], step, 1) if step else stats[i], packed)
    return packed


def merge_body(n_heads, chunk, span, keep, got, stat, gstat, out, ostat):
    mine = pack_rows([stat[i] for i in range(span)], span, chunk, 1)
    theirs = pack_rows([gstat[i] for i in range(span)], span, chunk, 3)
    t0, d0, t1, d1 = mine[:n_heads], mine[n_heads:], theirs[:n_heads], theirs[n_heads:]
    top = jnp.maximum(t0, t1)
    w0 = jnp.exp2(t0 - top)
    w1 = jnp.exp2(t1 - top)
    ostat[0] = jnp.concatenate([top, w0 * d0 + w1 * d1], axis=0)
    w = jnp.concatenate([w0, w1], axis=0).T
    tokens = span * chunk
    for h in range(n_heads):
        cols = slice(h * HD, (h + 1) * HD)
        val = keep[:, :, cols].reshape(tokens, HD) * w[:, h:h + 1]
        val = val + got[:, :, cols].reshape(tokens, HD) * w[:, n_heads + h:n_heads + h + 1]
        out[:, :, cols] = val.reshape(span, chunk, HD)


def merge(keep, got, stat, gstat, n_heads, row, rows):
    _, chunk2, width = keep.shape
    chunk = chunk2 // 2
    span = 4
    lead = row // span
    half = pl.BlockSpec((span, chunk, width), lambda i: (i + lead, 1, 0))
    stats = pl.BlockSpec((span, 2 * n_heads, 4 * chunk), lambda i: (i + lead, 0, 0))
    return pl.pallas_call(
        functools.partial(merge_body, n_heads, chunk, span),
        grid=(rows // span,),
        in_specs=[half, half, stats, stats],
        out_specs=[pl.BlockSpec((span, chunk, width), lambda i: (i, 0, 0)),
                   pl.BlockSpec((1, 2 * n_heads, 4 * chunk), lambda i: (i, 0, 0))],
        out_shape=[jax.ShapeDtypeStruct((rows, chunk, width), jnp.float32),
                   jax.ShapeDtypeStruct((rows // span, 2 * n_heads, 4 * chunk), jnp.float32)],
        compiler_params=params(),
        cost_estimate=cost(rows * 0.3, rows * chunk * width * 12),
        name="merge",
    )(keep, got, stat, gstat)


def finish_body(n_heads, chunk, span, keep, got, far, stat, gstat, fstat, out):
    sets = [pack_rows([stat[i] for i in range(span)], span, chunk, 0),
            pack_rows([gstat[i] for i in range(span)], span, chunk, 2), fstat[0]]
    pairs = [(x[:n_heads], x[n_heads:]) for x in sets]
    top = jnp.maximum(jnp.maximum(pairs[0][0], pairs[1][0]), pairs[2][0])
    ws = [jnp.exp2(t - top) for t, _ in pairs]
    den = ws[0] * pairs[0][1] + ws[1] * pairs[1][1] + ws[2] * pairs[2][1]
    inv = 1.0 / den
    w = jnp.concatenate([x * inv for x in ws], axis=0).T
    tokens = span * chunk
    for h in range(n_heads):
        cols = slice(h * HD, (h + 1) * HD)
        val = keep[:, :, cols].reshape(tokens, HD) * w[:, h:h + 1]
        val = val + got[:, :, cols].reshape(tokens, HD) * w[:, n_heads + h:n_heads + h + 1]
        val = val + far[:, :, cols].reshape(tokens, HD) * w[:, 2 * n_heads + h:2 * n_heads + h + 1]
        out[:, :, cols] = val.astype(jnp.bfloat16).reshape(span, chunk, HD)


def finish(keep, got, far, stat, gstat, fstat, n_heads, row, rows):
    _, chunk2, width = keep.shape
    chunk = chunk2 // 2
    span = 4
    lead = row // span
    half = pl.BlockSpec((span, chunk, width), lambda i: (i + lead, 0, 0))
    plain = pl.BlockSpec((span, chunk, width), lambda i: (i, 0, 0))
    stats = pl.BlockSpec((span, 2 * n_heads, 4 * chunk), lambda i: (i + lead, 0, 0))
    return pl.pallas_call(
        functools.partial(finish_body, n_heads, chunk, span),
        grid=(rows // span,),
        in_specs=[half, half, plain, stats, stats, pl.BlockSpec((1, 2 * n_heads, 4 * chunk), lambda i: (i, 0, 0))],
        out_specs=plain,
        out_shape=jax.ShapeDtypeStruct((rows, chunk, width), jnp.bfloat16),
        compiler_params=params(),
        cost_estimate=cost(rows * 0.4, rows * chunk * width * 14),
        name="finish",
    )(keep, got, far, stat, gstat, fstat)


def chain(o, steps):
    total = None
    for at, part in steps:
        term = jnp.dot(o[:, pl.ds(at, part.shape[0])], part[...], preferred_element_type=jnp.float32)
        total = term if total is None else total + term
    return total


def own_steps(w_own, core, half):
    steps = []
    for side in (core, 1 - core):
        at = 0
        for size in PIECES:
            lo = pl.multiple_of(side * half + at, HD)
            steps.append((lo, w_own.at[pl.ds(lo, size)]))
            at += size
    return steps


def peer_steps(near, far, core, half):
    steps = []
    for side, parts in ((core, near), (1 - core, far)):
        at = 0
        for size, part in zip(PIECES, parts):
            steps.append((pl.multiple_of(side * half + at, HD), part))
            at += size
    return steps


def gather_rows(dst, pieces):
    at = 0
    for piece in pieces:
        size = piece.shape[0]
        dst[at:at + size, :] = piece[...]
        at += size


def own_body(n, half, sc_ref, *refs):
    o_in = refs[:n]
    w_own, out, o = refs[n:]
    core = sc_ref[0] % 2

    @pl.when(pl.program_id(0) == 0)
    def _():
        gather_rows(o, o_in)

    out[...] = chain(o, own_steps(w_own, core, half))


def project_body(n, half, steps, block, row_starts, sc_ref, *refs):
    p = len(PIECES)
    j = pl.program_id(0)
    core = sc_ref[0] % 2
    ro_in, refs = refs[:n], refs[n:]
    near, far, refs = refs[:p], refs[p:2 * p], refs[2 * p:]
    x_hbm, gain, ready = refs[:3]
    out_hbm, ro, x, acc, ssq, sem, out_sem = refs[-7:]
    sizes = [r.shape[0] for r in ro_in]
    spots = [sum(sizes[:k]) for k in range(n)]

    def copies(out):
        made = []
        for k in range(n):
            there = pl.ds(row_starts[k], sizes[k])
            here = x.at[pl.ds(spots[k], sizes[k])]
            if out:
                made.append(pltpu.make_async_copy(here, out_hbm.at[there], out_sem.at[k]))
            else:
                made.append(pltpu.make_async_copy(x_hbm.at[there], here, sem.at[k]))
        return made

    @pl.when(j == 0)
    def _():
        for c in copies(False):
            c.start()
        gather_rows(ro, ro_in)

    a = ready[...] + chain(ro, peer_steps(near, far, core, half))
    acc[j] = a
    sq = jnp.sum(a * a, axis=-1, keepdims=True)
    ssq[...] = jnp.where(j == 0, sq, ssq[...] + sq)

    @pl.when(j == steps - 1)
    def _():
        for c in copies(False):
            c.wait()
        inv = lax.rsqrt(ssq[...] / (steps * block) + NORM_EPS)
        for k in range(steps):
            cols = slice(k * block, (k + 1) * block)
            y = x[:, cols].astype(jnp.float32) + acc[k] * inv * gain[:, cols].astype(jnp.float32)
            x[:, cols] = y.astype(jnp.bfloat16)
        for c in copies(True):
            c.start()
        for c in copies(True):
            c.wait()


def rows_spec(pieces):
    return [pl.BlockSpec(o.shape, lambda j, s: (0, 0), pipeline_mode=pl.Buffered(1)) for o in pieces]


def project_own(scalars, o_list, w_own):
    tokens, width = sum(o.shape[0] for o in o_list), o_list[0].shape[1]
    model = w_own.shape[1]
    block = P_BLOCK
    return pl.pallas_call(
        functools.partial(own_body, len(o_list), width // 2),
        grid_spec=pltpu.PrefetchScalarGridSpec(
            num_scalar_prefetch=1, grid=(model // block,),
            in_specs=rows_spec(o_list) + [pl.BlockSpec((width, block), lambda j, s: (0, j))],
            out_specs=pl.BlockSpec((tokens, block), lambda j, s: (0, j)),
            scratch_shapes=[pltpu.VMEM((tokens, width), jnp.bfloat16)]),
        out_shape=jax.ShapeDtypeStruct((tokens, model), jnp.float32),
        compiler_params=params(),
        cost_estimate=cost(6 + tokens * 0.02, 2 * width * model),
        name="project_own",
    )(scalars, *o_list, w_own)


def project(scalars, ready, ro_list, near, far, x, gain, row_starts, so_far):
    n = len(ro_list)
    tokens, width = sum(o.shape[0] for o in ro_list), ro_list[0].shape[1]
    model = x.shape[1]
    block = P_BLOCK
    steps = model // block
    anywhere = pl.BlockSpec(memory_space=pl.ANY)
    w_specs = [pl.BlockSpec((p.shape[0], block), lambda j, s: (0, j)) for p in list(near) + list(far)]
    specs = rows_spec(ro_list) + w_specs + [anywhere, pl.BlockSpec((1, model), lambda j, s: (0, 0)),
                                            pl.BlockSpec((tokens, block), lambda j, s: (0, j))]
    args = [*ro_list, *near, *far, x, gain, ready]
    alias = {}
    if so_far is not None:
        alias = {1 + len(args): 0}
        specs.append(anywhere)
        args.append(so_far)
    return pl.pallas_call(
        functools.partial(project_body, n, width // 2, steps, block, row_starts),
        grid_spec=pltpu.PrefetchScalarGridSpec(
            num_scalar_prefetch=1, grid=(steps,), in_specs=specs, out_specs=anywhere,
            scratch_shapes=[pltpu.VMEM((tokens, width), jnp.bfloat16), pltpu.VMEM((tokens, model), jnp.bfloat16),
                            pltpu.VMEM((steps, tokens, block), jnp.float32), pltpu.VMEM((tokens, 1), jnp.float32),
                            pltpu.SemaphoreType.DMA((n,)), pltpu.SemaphoreType.DMA((n,))]),
        out_shape=jax.ShapeDtypeStruct(x.shape, jnp.bfloat16),
        input_output_aliases=alias,
        compiler_params=params(),
        cost_estimate=cost(10 + tokens * 0.02, 2 * width * model),
        name="project",
    )(scalars, *args)


def solution(mesh):
    tp_size = mesh.shape['tp']
    OTHER_CHIP = [(0, 2), (2, 0), (1, 3), (3, 1)]
    OTHER_CORE = [(0, 1), (1, 0), (2, 3), (3, 2)]
    OTHER_HALF = [(0, 1), (1, 0)]

    def local_step(x_chunk, w_query, w_key, w_value, w_out, q_gain, k_gain, post_gain, cache_k, cache_v, prefix_len):
        rows, chunk, model = x_chunk.shape
        n_heads = cache_k.shape[2]
        width = n_heads * HD
        total_width = width * tp_size
        cp = lax.axis_index('cp')
        tp = lax.axis_index('tp')
        core = cp % 2
        tokens = x_chunk.reshape(rows * chunk, model)
        scalars = jnp.concatenate([cp[None], prefix_len]).astype(jnp.int32)
        places = jnp.stack([cp, tp]).astype(jnp.int32)
        positions = prefix_len[:, None] + cp * chunk + jnp.arange(chunk, dtype=jnp.int32)[None, :]
        inv_freq = ROPE_BASE ** (-(jnp.arange(HD // 2, dtype=jnp.float32) * 2.0 / HD))
        angles = positions.astype(jnp.float32).reshape(-1, 1) * inv_freq[None, :]
        cos_h, sin_h = jnp.cos(angles), jnp.sin(angles)
        cos = jnp.concatenate([cos_h, cos_h], axis=-1)
        sin = jnp.concatenate([-sin_h, sin_h], axis=-1)
        qg = q_gain.astype(jnp.float32)[None]
        kg = k_gain.astype(jnp.float32)[None]
        pg = post_gain[None]

        def after(value, done):
            return lax.optimization_barrier((value, done))[0]

        def swap(own):
            return own, lax.ppermute(own, 'tp', OTHER_HALF)

        def w_slice(n, done):
            lo = core * (width // 2) + sum(PIECES[:n])
            return lax.dynamic_slice_in_dim(after(w_out, done), lo, PIECES[n], axis=0)

        def rotated(raw, sums, gain, row0, count, raw_row0, done):
            return rope(raw, *sums, after(gain, done), cos, sin, row0 * chunk, total_width, count * chunk, raw_row0 * chunk)

        def spread(q):
            q = q.reshape(-1, chunk, width)
            q_chip = lax.ppermute(q, 'cp', OTHER_CHIP)
            q_core = lax.ppermute(q, 'cp', OTHER_CORE)
            return q, q_chip, q_core, lax.ppermute(q_chip, 'cp', OTHER_CORE)

        f32 = jnp.float32
        split, first_rows = GROUPS[0]
        raw0, own0 = dense(tokens, w_query, split * chunk, first_rows * chunk)
        sums0 = swap(own0)
        ws0 = w_slice(0, own0)
        q0 = rotated(raw0, sums0, qg, split, first_rows, split, ws0)
        q_sets = [spread(q0)]
        raw1, own1 = dense(after(tokens, q0), w_query, 0, split * chunk)
        sums1 = swap(own1)
        ws1 = w_slice(1, own1)
        last = ws1
        for g in range(1, len(GROUPS)):
            last = rotated(raw1, sums1, qg, *GROUPS[g], 0, last)
            q_sets.append(spread(last))
        wn0 = lax.ppermute(after(ws0, own1), 'tp', OTHER_HALF)
        k_raw = jnp.dot(after(tokens, last), w_key, preferred_element_type=f32)
        k_sums = swap(jnp.sum(k_raw * k_raw, axis=-1)[None])
        bf16 = jnp.bfloat16
        v_first = dense(after(tokens, k_sums[0]), w_value, split * chunk, first_rows * chunk, bf16)[0]
        k_first = rotated(k_raw, k_sums, kg, split, first_rows, 0, v_first)
        wn1 = lax.ppermute(after(ws1, k_sums[0]), 'tp', OTHER_HALF)
        near = (wn0, wn1)
        far_w = tuple(lax.ppermute(w, 'cp', OTHER_CORE) for w in near)
        v_new = [v_first.reshape(-1, chunk, width)]
        k_new = [k_first.reshape(-1, chunk, width)]

        parts, merged, o_mine, o_peer = {}, {}, {}, {}

        def attend(u, done):
            g, off, count = ATTEND[u]
            row0 = GROUPS[g][0] + off
            side, kv_row = (1, row0) if g else (0, off)
            keep, give, stat = attention(after(scalars, done), q_sets[g], off, count, cache_k, cache_v,
                                      k_new[side], kv_row, v_new[side], kv_row, row0)
            parts[u] = (keep, give, stat, lax.ppermute(give, 'cp', OTHER_CORE), lax.ppermute(stat, 'cp', OTHER_CORE))
            return stat

        def combine(m, done):
            u, off, count = MERGE[m]
            keep, _, stat, got, gstat = parts[u]
            send, sstat = merge(keep, got, after(stat, done), gstat, n_heads, off, count)
            merged[m] = (lax.ppermute(send, 'cp', OTHER_CHIP), lax.ppermute(sstat, 'cp', OTHER_CHIP))
            return sstat

        def close(m, done):
            u, off, count = MERGE[m]
            keep, _, stat, got, gstat = parts[u]
            o = finish(keep, got, merged[m][0], after(stat, done), gstat, merged[m][1], n_heads, off, count)
            o_mine[m] = o.reshape(-1, width)
            o_peer[m] = lax.ppermute(o_mine[m], 'tp', OTHER_HALF)
            return o

        def row_of(m):
            u, off, _ = MERGE[m]
            g, a_off, _ = ATTEND[u]
            return (GROUPS[g][0] + a_off + off) * chunk

        def mix(n, ready, so_far=None):
            groups = P_GROUPS[n]
            return project(places, ready, [o_peer[g] for g in groups],
                          near, far_w, tokens, pg, tuple(row_of(m) for m in groups), so_far)

        def own_part(n, done):
            return project_own(after(places, done), [o_mine[g] for g in P_GROUPS[n]], w_out)

        shape = (rows, chunk, n_heads, HD)
        last = attend(0, k_first)
        last = attend(1, last)
        last = combine(0, last)
        v_rest = dense(after(tokens, last), w_value, 0, split * chunk, bf16)[0]
        v_new.append(v_rest.reshape(-1, chunk, width))
        last = combine(1, v_rest)
        k_rest = rotated(k_raw, k_sums, kg, 0, split, 0, last)
        k_new.append(k_rest.reshape(-1, chunk, width))
        last = attend(2, k_rest)
        chunk_k = jnp.concatenate([after(k_rest, last), k_first], axis=0).reshape(shape)
        last = combine(2, chunk_k)
        last = close(0, last)
        last = attend(3, last)
        chunk_v = jnp.concatenate([after(v_rest, last), v_first], axis=0).reshape(shape)
        last = close(1, chunk_v)
        last = combine(3, last)
        last = attend(4, last)
        last = close(2, last)
        last = combine(4, last)
        last = combine(5, last)
        ready = own_part(0, last)
        last = close(3, ready)
        block_out = mix(0, after(ready, last))
        last = close(4, block_out)
        last = close(5, last)
        block_out = mix(1, own_part(1, last), block_out)
        return block_out.reshape(rows, chunk, model), chunk_k, chunk_v

    x_spec = P('dp', 'cp', None)
    head_spec = P('dp', 'cp', 'tp', None)
    in_specs = (x_spec, P(None, 'tp'), P(None, 'tp'), P(None, 'tp'), P('tp', None), P('tp'), P('tp'), P(None), head_spec, head_spec, P('dp'))
    out_specs = (x_spec, head_spec, head_spec)

    return jax.shard_map(local_step, mesh=mesh, in_specs=in_specs, out_specs=out_specs, check_vma=False)
```

```python
import functools

import jax
import jax.numpy as jnp
from jax import lax
from jax.experimental import pallas as pl
from jax.experimental.pallas import tpu as pltpu
from jax.sharding import PartitionSpec as P

NORM_EPS = 1e-6
ROPE_BASE = 500000.0
NEG = -1e30
FLOOR = -5e29
LOG2E = 1.4426950408889634
HD = 128
LAG = 2
ROPE_BLOCK = 384
P_BLOCK = 1024
GROUPS = ((24, 8), (0, 8), (8, 8), (16, 8))
ATTEND = ((0, 0, 4), (0, 4, 4), (1, 0, 8), (2, 0, 8), (3, 0, 8))
MERGE = ((0, 0, 4), (1, 0, 4), (2, 0, 8), (3, 0, 8), (4, 0, 4), (4, 4, 4))
P_GROUPS = ((0, 1, 2), (3, 4, 5))
PIECES = (256, 768)
VMEM_LIMIT = 60 * 1024 * 1024


def cost(micros, moved):
    return pl.CostEstimate(flops=int(micros * 9e8), bytes_accessed=moved, transcendentals=0)


def params():
    return pltpu.CompilerParams(dimension_semantics=("arbitrary",), vmem_limit_bytes=VMEM_LIMIT)


def dense_body(steps, x, w, out, sums, acc):
    j = pl.program_id(0)
    r = jnp.dot(x[...], w[...], preferred_element_type=jnp.float32)
    out[...] = r.astype(out.dtype)
    sq = r * r
    part = sq[:, :HD]
    for c in range(HD, sq.shape[1], HD):
        part = part + sq[:, c:c + HD]
    acc[...] = jnp.where(j == 0, part, acc[...] + part)

    @pl.when(j == steps - 1)
    def _():
        for t in range(0, acc.shape[0], HD):
            sums[:, t:t + HD] = jnp.sum(acc[t:t + HD, :].T, axis=0, keepdims=True)


def dense(x, w, row0, tokens, dtype=jnp.float32):
    model, width = w.shape
    block = 512
    steps = width // block
    row_block = row0 // tokens
    return pl.pallas_call(
        functools.partial(dense_body, steps),
        grid=(steps,),
        in_specs=[pl.BlockSpec((tokens, model), lambda j: (row_block, 0), pipeline_mode=pl.Buffered(1)),
                  pl.BlockSpec((model, block), lambda j: (0, j))],
        out_specs=[pl.BlockSpec((tokens, block), lambda j: (0, j)), pl.BlockSpec((1, tokens), lambda j: (0, 0))],
        out_shape=[jax.ShapeDtypeStruct((tokens, width), dtype), jax.ShapeDtypeStruct((1, tokens), jnp.float32)],
        scratch_shapes=[pltpu.VMEM((tokens, HD), jnp.float32)],
        compiler_params=params(),
        cost_estimate=cost(8 + tokens * 0.015, model * width * 2),
        name="dense",
    )(x, w)


def rope_body(total_width, n_heads, raw, own, peer, gain, cos, sin, out):
    inv = lax.rsqrt((own[...] + peer[...]) / total_width + NORM_EPS)
    inv = jnp.concatenate([jnp.broadcast_to(inv[:, i:i + HD], (HD, HD)).T for i in range(0, inv.shape[1], HD)], axis=0)
    cos_t = cos[...]
    sin_t = sin[...]
    for h in range(n_heads):
        cols = slice(h * HD, (h + 1) * HD)
        u = raw[:, cols] * inv * gain[:, cols]
        out[:, cols] = (u * cos_t + pltpu.roll(u, HD // 2, 1) * sin_t).astype(jnp.bfloat16)


def rope(raw, own, peer, gain, cos, sin, row0, total_width, tokens, raw_row0):
    width = raw.shape[1]
    block = ROPE_BLOCK if tokens % ROPE_BLOCK == 0 else 128
    base = row0 // block
    off = (row0 - raw_row0) // block
    return pl.pallas_call(
        functools.partial(rope_body, total_width, width // HD),
        grid=(tokens // block,),
        in_specs=[pl.BlockSpec((block, width), lambda i: (i + off, 0)),
                  pl.BlockSpec((1, block), lambda i: (0, i + off)),
                  pl.BlockSpec((1, block), lambda i: (0, i + off)),
                  pl.BlockSpec((1, width), lambda i: (0, 0)),
                  pl.BlockSpec((block, HD), lambda i: (i + base, 0)),
                  pl.BlockSpec((block, HD), lambda i: (i + base, 0))],
        out_specs=pl.BlockSpec((block, width), lambda i: (i, 0)),
        out_shape=jax.ShapeDtypeStruct((tokens, width), jnp.bfloat16),
        compiler_params=params(),
        cost_estimate=cost(tokens * 0.005, tokens * width * 6),
        name="rope",
    )(raw, own, peer, gain, cos, sin)


def attn_body(n_heads, row0, chunk, slots, pitch, sc_ref, qa, qb, qc, qd, ck, cv, kc, vc, keep, give, stat, ks, vs):
    b = pl.program_id(0)
    cp = sc_ref[0]
    valid_len = sc_ref[1 + row0 + b]
    tokens = 4 * chunk
    keys = slots + chunk
    for t in range(slots):
        ks[t * pitch:t * pitch + n_heads, :] = ck[0, t].astype(jnp.float32)
        vs[t * pitch:t * pitch + n_heads, :] = cv[0, t].astype(jnp.float32)
    row = lax.broadcasted_iota(jnp.int32, (keys, tokens), 0)
    col = lax.broadcasted_iota(jnp.int32, (keys, tokens), 1)
    part = col // chunk
    rel = jnp.where(part == 1, 2, jnp.where(part == 2, 1, part))
    query = jnp.bitwise_xor(rel, cp) * chunk + col % chunk
    chunk_key = cp * chunk + row - slots
    ok = jnp.where(row < slots, row + cp * slots - valid_len, chunk_key - query - 1) < 0
    scale = HD ** -0.5 * LOG2E
    contract_last = (((1,), (1,)), ((), ()))
    contract_first = (((0,), (0,)), ((), ()))

    def cols(h):
        return slice(h * HD, (h + 1) * HD)

    def scores(h):
        q = jnp.concatenate([qa[0, :, cols(h)], qb[0, :, cols(h)], qc[0, :, cols(h)], qd[0, :, cols(h)]], axis=0)
        k = jnp.concatenate([ks[pl.ds(h, slots, stride=pitch), :].astype(jnp.bfloat16), kc[0, :, cols(h)]], axis=0)
        return lax.dot_general(k, q, contract_last, preferred_element_type=jnp.float32)

    def soft(h, s):
        s = jnp.where(ok, s * scale, NEG)
        top = jnp.maximum(jnp.max(s, axis=0, keepdims=True), FLOOR)
        p = jnp.exp2(s - top)
        den = jnp.sum(p, axis=0, keepdims=True)
        for at, val in ((h, top), (n_heads + h, den)):
            stat[0, at:at + 1, :] = val
            give[0, at:at + 1, n_heads * HD:] = val
        return p.astype(jnp.bfloat16)

    def values(h, p):
        v = jnp.concatenate([vs[pl.ds(h, slots, stride=pitch), :].astype(jnp.bfloat16), vc[0, :, cols(h)]], axis=0)
        num = lax.dot_general(p, v, contract_first, preferred_element_type=jnp.float32)
        keep[0, :, cols(h)] = num[:2 * chunk]
        give[0, :, cols(h)] = num[2 * chunk:]

    s_live, p_live = {}, {}
    for step in range(n_heads + 2 * LAG):
        if step < n_heads:
            s_live[step] = scores(step)
        h = step - LAG
        if 0 <= h < n_heads:
            p_live[h] = soft(h, s_live.pop(h))
        h = step - 2 * LAG
        if 0 <= h < n_heads:
            values(h, p_live.pop(h))


def attention(scalars, q_parts, q_row, rows, cache_k, cache_v, k_new, k_row, v_new, v_row, row0):
    _, chunk, width = q_parts[0].shape
    _, slots, n_heads, _ = cache_k.shape
    pitch = n_heads + 8
    q_spec = pl.BlockSpec((1, chunk, width), lambda b, s: (b + q_row, 0, 0))
    k_spec = pl.BlockSpec((1, chunk, width), lambda b, s: (b + k_row, 0, 0))
    v_spec = pl.BlockSpec((1, chunk, width), lambda b, s: (b + v_row, 0, 0))
    cache_spec = pl.BlockSpec((1, slots, n_heads, HD), lambda b, s: (b + row0, 0, 0, 0))
    out_spec = pl.BlockSpec((1, 2 * chunk, width), lambda b, s: (b, 0, 0))
    stat_spec = pl.BlockSpec((1, 2 * n_heads, 4 * chunk), lambda b, s: (b, 0, 0))
    give_spec = pl.BlockSpec((1, 2 * chunk, width + 4 * chunk), lambda b, s: (b, 0, 0))
    out = jax.ShapeDtypeStruct((rows, 2 * chunk, width), jnp.float32)
    give = jax.ShapeDtypeStruct((rows, 2 * chunk, width + 4 * chunk), jnp.float32)
    return pl.pallas_call(
        functools.partial(attn_body, n_heads, row0, chunk, slots, pitch),
        grid_spec=pltpu.PrefetchScalarGridSpec(
            num_scalar_prefetch=1, grid=(rows,),
            in_specs=[q_spec] * 4 + [cache_spec] * 2 + [k_spec, v_spec],
            out_specs=[out_spec, give_spec, stat_spec],
            scratch_shapes=[pltpu.VMEM((slots * pitch, HD), jnp.float32)] * 2),
        out_shape=[out, give, jax.ShapeDtypeStruct((rows, 2 * n_heads, 4 * chunk), jnp.float32)],
        compiler_params=params(),
        cost_estimate=cost(rows * 3.9, rows * slots * width * 6),
        name="attention",
    )(scalars, *q_parts, cache_k, cache_v, k_new, v_new)


def pack_rows(stats, span, chunk, shift):
    lane = lax.broadcasted_iota(jnp.int32, stats[0].shape, 1) // chunk
    width = stats[0].shape[1]
    packed = stats[0] if shift == 0 else pltpu.roll(stats[0], (-shift * chunk) % width, 1)
    for i in range(1, span):
        step = ((i - shift) * chunk) % width
        packed = jnp.where(lane == i, pltpu.roll(stats[i], step, 1) if step else stats[i], packed)
    return packed


def merge_body(n_heads, chunk, span, keep, got, stat, gstat, out, ostat):
    mine = pack_rows([stat[i] for i in range(span)], span, chunk, 1)
    theirs = pack_rows([gstat[i] for i in range(span)], span, chunk, 3)
    t0, d0, t1, d1 = mine[:n_heads], mine[n_heads:], theirs[:n_heads], theirs[n_heads:]
    top = jnp.maximum(t0, t1)
    w0 = jnp.exp2(t0 - top)
    w1 = jnp.exp2(t1 - top)
    ostat[0] = jnp.concatenate([top, w0 * d0 + w1 * d1], axis=0)
    w = jnp.concatenate([w0, w1], axis=0).T
    tokens = span * chunk
    for h in range(n_heads):
        cols = slice(h * HD, (h + 1) * HD)
        val = keep[:, :, cols].reshape(tokens, HD) * w[:, h:h + 1]
        val = val + got[:, :, cols].reshape(tokens, HD) * w[:, n_heads + h:n_heads + h + 1]
        out[:, :, cols] = val.reshape(span, chunk, HD)


def merge(keep, got, stat, gstat, n_heads, row, rows):
    _, chunk2, width = keep.shape
    chunk = chunk2 // 2
    span = 4
    lead = row // span
    half = pl.BlockSpec((span, chunk, width), lambda i: (i + lead, 1, 0))
    stats = pl.BlockSpec((span, 2 * n_heads, 4 * chunk), lambda i: (i + lead, 0, 0))
    given = pl.BlockSpec((span, 2 * n_heads, 4 * chunk), lambda i: (i + lead, 0, width // (4 * chunk)))
    return pl.pallas_call(
        functools.partial(merge_body, n_heads, chunk, span),
        grid=(rows // span,),
        in_specs=[half, half, stats, given],
        out_specs=[pl.BlockSpec((span, chunk, width), lambda i: (i, 0, 0)),
                   pl.BlockSpec((1, 2 * n_heads, 4 * chunk), lambda i: (i, 0, 0))],
        out_shape=[jax.ShapeDtypeStruct((rows, chunk, width), jnp.float32),
                   jax.ShapeDtypeStruct((rows // span, 2 * n_heads, 4 * chunk), jnp.float32)],
        compiler_params=params(),
        cost_estimate=cost(rows * 0.3, rows * chunk * width * 12),
        name="merge",
    )(keep, got, stat, gstat)


def finish_body(n_heads, chunk, span, keep, got, far, stat, gstat, fstat, out):
    sets = [pack_rows([stat[i] for i in range(span)], span, chunk, 0),
            pack_rows([gstat[i] for i in range(span)], span, chunk, 2), fstat[0]]
    pairs = [(x[:n_heads], x[n_heads:]) for x in sets]
    top = jnp.maximum(jnp.maximum(pairs[0][0], pairs[1][0]), pairs[2][0])
    ws = [jnp.exp2(t - top) for t, _ in pairs]
    den = ws[0] * pairs[0][1] + ws[1] * pairs[1][1] + ws[2] * pairs[2][1]
    inv = 1.0 / den
    w = jnp.concatenate([x * inv for x in ws], axis=0).T
    tokens = span * chunk
    for h in range(n_heads):
        cols = slice(h * HD, (h + 1) * HD)
        val = keep[:, :, cols].reshape(tokens, HD) * w[:, h:h + 1]
        val = val + got[:, :, cols].reshape(tokens, HD) * w[:, n_heads + h:n_heads + h + 1]
        val = val + far[:, :, cols].reshape(tokens, HD) * w[:, 2 * n_heads + h:2 * n_heads + h + 1]
        out[:, :, cols] = val.astype(jnp.bfloat16).reshape(span, chunk, HD)


def finish(keep, got, far, stat, gstat, fstat, n_heads, row, rows):
    _, chunk2, width = keep.shape
    chunk = chunk2 // 2
    span = 4
    lead = row // span
    half = pl.BlockSpec((span, chunk, width), lambda i: (i + lead, 0, 0))
    plain = pl.BlockSpec((span, chunk, width), lambda i: (i, 0, 0))
    stats = pl.BlockSpec((span, 2 * n_heads, 4 * chunk), lambda i: (i + lead, 0, 0))
    given = pl.BlockSpec((span, 2 * n_heads, 4 * chunk), lambda i: (i + lead, 0, width // (4 * chunk)))
    return pl.pallas_call(
        functools.partial(finish_body, n_heads, chunk, span),
        grid=(rows // span,),
        in_specs=[half, half, plain, stats, given, pl.BlockSpec((1, 2 * n_heads, 4 * chunk), lambda i: (i, 0, 0))],
        out_specs=plain,
        out_shape=jax.ShapeDtypeStruct((rows, chunk, width), jnp.bfloat16),
        compiler_params=params(),
        cost_estimate=cost(rows * 0.4, rows * chunk * width * 14),
        name="finish",
    )(keep, got, far, stat, gstat, fstat)


def chain(o, steps):
    total = None
    for at, part in steps:
        term = jnp.dot(o[:, pl.ds(at, part.shape[0])], part[...], preferred_element_type=jnp.float32)
        total = term if total is None else total + term
    return total


def own_steps(w_own, core, half):
    steps = []
    for side in (core, 1 - core):
        at = 0
        for size in PIECES:
            lo = pl.multiple_of(side * half + at, HD)
            steps.append((lo, w_own.at[pl.ds(lo, size)]))
            at += size
    return steps


def peer_steps(near, far, core, half):
    steps = []
    for side, parts in ((core, near), (1 - core, far)):
        at = 0
        for size, part in zip(PIECES, parts):
            steps.append((pl.multiple_of(side * half + at, HD), part))
            at += size
    return steps


def gather_rows(dst, pieces):
    at = 0
    for piece in pieces:
        size = piece.shape[0]
        dst[at:at + size, :] = piece[...]
        at += size


def own_body(n, half, sc_ref, *refs):
    o_in = refs[:n]
    w_own, out, o = refs[n:]
    core = sc_ref[0] % 2

    @pl.when(pl.program_id(0) == 0)
    def _():
        gather_rows(o, o_in)

    out[...] = chain(o, own_steps(w_own, core, half))


def project_body(n, half, steps, block, row_starts, sc_ref, *refs):
    p = len(PIECES)
    j = pl.program_id(0)
    core = sc_ref[0] % 2
    ro_in, refs = refs[:n], refs[n:]
    near, far, refs = refs[:p], refs[p:2 * p], refs[2 * p:]
    x_hbm, gain, ready = refs[:3]
    out_hbm, ro, x, acc, ssq, sem, out_sem = refs[-7:]
    sizes = [r.shape[0] for r in ro_in]
    spots = [sum(sizes[:k]) for k in range(n)]

    def copies(out):
        made = []
        for k in range(n):
            there = pl.ds(row_starts[k], sizes[k])
            here = x.at[pl.ds(spots[k], sizes[k])]
            if out:
                made.append(pltpu.make_async_copy(here, out_hbm.at[there], out_sem.at[k]))
            else:
                made.append(pltpu.make_async_copy(x_hbm.at[there], here, sem.at[k]))
        return made

    @pl.when(j == 0)
    def _():
        for c in copies(False):
            c.start()
        gather_rows(ro, ro_in)

    a = ready[...] + chain(ro, peer_steps(near, far, core, half))
    acc[j] = a
    sq = jnp.sum(a * a, axis=-1, keepdims=True)
    ssq[...] = jnp.where(j == 0, sq, ssq[...] + sq)

    @pl.when(j == steps - 1)
    def _():
        for c in copies(False):
            c.wait()
        inv = lax.rsqrt(ssq[...] / (steps * block) + NORM_EPS)
        for k in range(steps):
            cols = slice(k * block, (k + 1) * block)
            y = x[:, cols].astype(jnp.float32) + acc[k] * inv * gain[:, cols].astype(jnp.float32)
            x[:, cols] = y.astype(jnp.bfloat16)
        for c in copies(True):
            c.start()
        for c in copies(True):
            c.wait()


def rows_spec(pieces):
    return [pl.BlockSpec(o.shape, lambda j, s: (0, 0), pipeline_mode=pl.Buffered(1)) for o in pieces]


def project_own(scalars, o_list, w_own):
    tokens, width = sum(o.shape[0] for o in o_list), o_list[0].shape[1]
    model = w_own.shape[1]
    block = P_BLOCK
    return pl.pallas_call(
        functools.partial(own_body, len(o_list), width // 2),
        grid_spec=pltpu.PrefetchScalarGridSpec(
            num_scalar_prefetch=1, grid=(model // block,),
            in_specs=rows_spec(o_list) + [pl.BlockSpec((width, block), lambda j, s: (0, j))],
            out_specs=pl.BlockSpec((tokens, block), lambda j, s: (0, j)),
            scratch_shapes=[pltpu.VMEM((tokens, width), jnp.bfloat16)]),
        out_shape=jax.ShapeDtypeStruct((tokens, model), jnp.float32),
        compiler_params=params(),
        cost_estimate=cost(6 + tokens * 0.02, 2 * width * model),
        name="project_own",
    )(scalars, *o_list, w_own)


def project(scalars, ready, ro_list, near, far, x, gain, row_starts, so_far):
    n = len(ro_list)
    tokens, width = sum(o.shape[0] for o in ro_list), ro_list[0].shape[1]
    model = x.shape[1]
    block = P_BLOCK
    steps = model // block
    anywhere = pl.BlockSpec(memory_space=pl.ANY)
    w_specs = [pl.BlockSpec((p.shape[0], block), lambda j, s: (0, j)) for p in list(near) + list(far)]
    specs = rows_spec(ro_list) + w_specs + [anywhere, pl.BlockSpec((1, model), lambda j, s: (0, 0)),
                                            pl.BlockSpec((tokens, block), lambda j, s: (0, j))]
    args = [*ro_list, *near, *far, x, gain, ready]
    alias = {}
    if so_far is not None:
        alias = {1 + len(args): 0}
        specs.append(anywhere)
        args.append(so_far)
    return pl.pallas_call(
        functools.partial(project_body, n, width // 2, steps, block, row_starts),
        grid_spec=pltpu.PrefetchScalarGridSpec(
            num_scalar_prefetch=1, grid=(steps,), in_specs=specs, out_specs=anywhere,
            scratch_shapes=[pltpu.VMEM((tokens, width), jnp.bfloat16), pltpu.VMEM((tokens, model), jnp.bfloat16),
                            pltpu.VMEM((steps, tokens, block), jnp.float32), pltpu.VMEM((tokens, 1), jnp.float32),
                            pltpu.SemaphoreType.DMA((n,)), pltpu.SemaphoreType.DMA((n,))]),
        out_shape=jax.ShapeDtypeStruct(x.shape, jnp.bfloat16),
        input_output_aliases=alias,
        compiler_params=params(),
        cost_estimate=cost(10 + tokens * 0.02, 2 * width * model),
        name="project",
    )(scalars, *args)


def solution(mesh):
    tp_size = mesh.shape['tp']
    OTHER_CHIP = [(0, 2), (2, 0), (1, 3), (3, 1)]
    OTHER_CORE = [(0, 1), (1, 0), (2, 3), (3, 2)]
    OTHER_HALF = [(0, 1), (1, 0)]

    def local_step(x_chunk, w_query, w_key, w_value, w_out, q_gain, k_gain, post_gain, cache_k, cache_v, prefix_len):
        rows, chunk, model = x_chunk.shape
        n_heads = cache_k.shape[2]
        width = n_heads * HD
        total_width = width * tp_size
        cp = lax.axis_index('cp')
        tp = lax.axis_index('tp')
        core = cp % 2
        tokens = x_chunk.reshape(rows * chunk, model)
        scalars = jnp.concatenate([cp[None], prefix_len]).astype(jnp.int32)
        places = jnp.stack([cp, tp]).astype(jnp.int32)
        positions = prefix_len[:, None] + cp * chunk + jnp.arange(chunk, dtype=jnp.int32)[None, :]
        inv_freq = ROPE_BASE ** (-(jnp.arange(HD // 2, dtype=jnp.float32) * 2.0 / HD))
        angles = positions.astype(jnp.float32).reshape(-1, 1) * inv_freq[None, :]
        cos_h, sin_h = jnp.cos(angles), jnp.sin(angles)
        cos = jnp.concatenate([cos_h, cos_h], axis=-1)
        sin = jnp.concatenate([-sin_h, sin_h], axis=-1)
        qg = q_gain.astype(jnp.float32)[None]
        kg = k_gain.astype(jnp.float32)[None]
        pg = post_gain[None]

        def after(value, done):
            return lax.optimization_barrier((value, done))[0]

        def swap(own):
            return own, lax.ppermute(own, 'tp', OTHER_HALF)

        def w_slice(n, done):
            lo = core * (width // 2) + sum(PIECES[:n])
            return lax.dynamic_slice_in_dim(after(w_out, done), lo, PIECES[n], axis=0)

        def rotated(raw, sums, gain, row0, count, raw_row0, done):
            return rope(raw, *sums, after(gain, done), cos, sin, row0 * chunk, total_width, count * chunk, raw_row0 * chunk)

        def spread(q):
            q = q.reshape(-1, chunk, width)
            q_chip = lax.ppermute(q, 'cp', OTHER_CHIP)
            q_core = lax.ppermute(q, 'cp', OTHER_CORE)
            return q, q_chip, q_core, lax.ppermute(q_chip, 'cp', OTHER_CORE)

        f32 = jnp.float32
        split, first_rows = GROUPS[0]
        raw0, own0 = dense(tokens, w_query, split * chunk, first_rows * chunk)
        sums0 = swap(own0)
        ws0 = w_slice(0, own0)
        q0 = rotated(raw0, sums0, qg, split, first_rows, split, ws0)
        q_sets = [spread(q0)]
        raw1, own1 = dense(after(tokens, q0), w_query, 0, split * chunk)
        sums1 = swap(own1)
        ws1 = w_slice(1, own1)
        last = ws1
        for g in range(1, len(GROUPS)):
            last = rotated(raw1, sums1, qg, *GROUPS[g], 0, last)
            q_sets.append(spread(last))
        wn0 = lax.ppermute(after(ws0, own1), 'tp', OTHER_HALF)
        k_raw = jnp.dot(after(tokens, last), w_key, preferred_element_type=f32)
        k_sums = swap(jnp.sum(k_raw * k_raw, axis=-1)[None])
        bf16 = jnp.bfloat16
        v_first = dense(after(tokens, k_sums[0]), w_value, split * chunk, first_rows * chunk, bf16)[0]
        k_first = rotated(k_raw, k_sums, kg, split, first_rows, 0, v_first)
        wn1 = lax.ppermute(after(ws1, k_sums[0]), 'tp', OTHER_HALF)
        near = (wn0, wn1)
        far_w = tuple(lax.ppermute(w, 'cp', OTHER_CORE) for w in near)
        v_new = [v_first.reshape(-1, chunk, width)]
        k_new = [k_first.reshape(-1, chunk, width)]

        parts, merged, o_mine, o_peer = {}, {}, {}, {}

        def attend(u, done):
            g, off, count = ATTEND[u]
            row0 = GROUPS[g][0] + off
            side, kv_row = (1, row0) if g else (0, off)
            keep, give, stat = attention(after(scalars, done), q_sets[g], off, count, cache_k, cache_v,
                                      k_new[side], kv_row, v_new[side], kv_row, row0)
            got = lax.ppermute(give, 'cp', OTHER_CORE)
            parts[u] = (keep, give, stat, got, got)
            return stat

        def combine(m, done):
            u, off, count = MERGE[m]
            keep, _, stat, got, gstat = parts[u]
            send, sstat = merge(keep, got, after(stat, done), gstat, n_heads, off, count)
            merged[m] = (lax.ppermute(send, 'cp', OTHER_CHIP), lax.ppermute(sstat, 'cp', OTHER_CHIP))
            return sstat

        def close(m, done):
            u, off, count = MERGE[m]
            keep, _, stat, got, gstat = parts[u]
            o = finish(keep, got, merged[m][0], after(stat, done), gstat, merged[m][1], n_heads, off, count)
            o_mine[m] = o.reshape(-1, width)
            o_peer[m] = lax.ppermute(o_mine[m], 'tp', OTHER_HALF)
            return o

        def row_of(m):
            u, off, _ = MERGE[m]
            g, a_off, _ = ATTEND[u]
            return (GROUPS[g][0] + a_off + off) * chunk

        def mix(n, ready, so_far=None):
            groups = P_GROUPS[n]
            return project(places, ready, [o_peer[g] for g in groups],
                          near, far_w, tokens, pg, tuple(row_of(m) for m in groups), so_far)

        def own_part(n, done):
            return project_own(after(places, done), [o_mine[g] for g in P_GROUPS[n]], w_out)

        shape = (rows, chunk, n_heads, HD)
        last = attend(0, k_first)
        last = attend(1, last)
        last = combine(0, last)
        v_rest = dense(after(tokens, last), w_value, 0, split * chunk, bf16)[0]
        v_new.append(v_rest.reshape(-1, chunk, width))
        last = combine(1, v_rest)
        k_rest = rotated(k_raw, k_sums, kg, 0, split, 0, last)
        k_new.append(k_rest.reshape(-1, chunk, width))
        last = attend(2, k_rest)
        chunk_k = jnp.concatenate([after(k_rest, last), k_first], axis=0).reshape(shape)
        last = combine(2, chunk_k)
        last = close(0, last)
        last = attend(3, last)
        chunk_v = jnp.concatenate([after(v_rest, last), v_first], axis=0).reshape(shape)
        last = close(1, chunk_v)
        last = combine(3, last)
        last = attend(4, last)
        last = close(2, last)
        last = combine(4, last)
        last = combine(5, last)
        ready = own_part(0, last)
        last = close(3, ready)
        block_out = mix(0, after(ready, last))
        last = close(4, block_out)
        last = close(5, last)
        block_out = mix(1, own_part(1, last), block_out)
        return block_out.reshape(rows, chunk, model), chunk_k, chunk_v

    x_spec = P('dp', 'cp', None)
    head_spec = P('dp', 'cp', 'tp', None)
    in_specs = (x_spec, P(None, 'tp'), P(None, 'tp'), P(None, 'tp'), P('tp', None), P('tp'), P('tp'), P(None), head_spec, head_spec, P('dp'))
    out_specs = (x_spec, head_spec, head_spec)

    return jax.shard_map(local_step, mesh=mesh, in_specs=in_specs, out_specs=out_specs, check_vma=False)
```
